128 devices in a mesh: gx: 4 (over y_lo, core), gy: 4 (over x), gz: 8 (over y_hi, z).
Axes of the slice: x: 4, y: 4 (y_hi: 2, y_lo: 2; y = y_hi * 2 + y_lo), z: 4, core: 2. Of those that a mesh axis runs over, the one named last changes fastest.
Arguments:
- right_side: float32 [16, 16, 32, 4, 256], P('gx', 'gy', 'gz'), may hold values from -80 to 80
- bond_blocks: float32 [13, 4, 4, 16, 16, 32], P(None, None, None, 'gx', 'gy', 'gz'), may hold values from -0.012 to 0.012
- bond_open: int32 [13, 16, 16, 32], P(None, 'gx', 'gy', 'gz'), may hold values 0 or 1
- onsite_blocks: float32 [4, 4, 16, 16, 32], P(None, None, 'gx', 'gy', 'gz'), may hold values from -0.012 to 0.012
- orbital_levels: float32 [4, 16, 16, 32], P(None, 'gx', 'gy', 'gz'), may hold values from 1.3 to 2.6
- column_shift: float32 [256], replicated, may hold values from 0.05 to 1
Outputs:
- solution: float32 [16, 16, 32, 4, 256], P('gx', 'gy', 'gz')
- residual: float32 [16, 16, 32, 4, 256], P('gx', 'gy', 'gz')
The draws below stay inside these ranges and needn't reach their ends.
All inputs are finite; a program needn't handle non-finite values. No bound on the sum of `bond_open` on one device may be relied on, other than what follows from the above.
Results may differ from the reference program's by a relative error of at most 0.0003.
Values sent between devices are 32-bit elements; how exact they have to be, the bound alone decides.
A program may use at most 192 MiB of HBM per device.

```python
import math
import jax
import jax.numpy as jnp
from jax import lax

ORB = 4
COLS = 256
BONDS = 13
ITERS = 3
NX = 16
NY = 16
NZ = 32


def draw_right_side(key, part):
    subkeys = jax.random.split(key, 3)
    full_shape = (NX, NY, NZ, ORB, COLS)
    along_x = jnp.arange(NX, dtype=jnp.float32) / NX
    along_y = jnp.arange(NY, dtype=jnp.float32) / NY
    along_z = jnp.arange(NZ, dtype=jnp.float32) / NZ
    position_ramp = jnp.exp(0.37 * (along_x[:, None, None] + along_y[None, :, None] + along_z[None, None, :]))
    atom_scale = jnp.exp(jax.random.uniform(subkeys[1], (NX, NY, NZ, ORB, 1), jnp.float32, math.log(0.3), math.log(3.0)))
    values = jnp.clip(jax.random.normal(subkeys[0], full_shape, jnp.float32), -4.0, 4.0)
    column_scale = jnp.exp(jax.random.uniform(subkeys[2], (COLS,), jnp.float32, math.log(0.5), math.log(5.0)))
    return (0.3 * values * atom_scale * column_scale * position_ramp[:, :, :, None, None]).astype(jnp.float32)


def set_ends(array, rng, least, largest):
    shape = array.shape
    place = [jax.random.randint(jax.random.fold_in(rng, axis), (), 0, shape[axis]) for axis in range(len(shape))]
    array = array.at[tuple(place)].set(least)
    longest = shape.index(max(shape))
    place[longest] = (place[longest] + 1) % shape[longest]
    return array.at[tuple(place)].set(largest)


def level_of(key, extent, pieces, smallest, high):
    factor_of, own = 1.0, jax.random.fold_in(key, 6)
    for axis_at, shards_of in pieces:
        steps = jnp.exp(jax.random.uniform(jax.random.fold_in(own, axis_at), (shards_of,), jnp.float32, smallest / len(pieces), high / len(pieces)))
        factor_of = factor_of * jnp.repeat(steps, extent[axis_at] // shards_of).reshape([-1 if axis == axis_at else 1 for axis in range(len(extent))])
    return factor_of


def setup_inputs(seed: int = 0) -> dict:
    keys = jax.random.split(jax.random.key(seed), 7)
    return {
        "right_side": draw_right_side(jax.random.fold_in(keys[6], 71), 0),
        "bond_blocks": jnp.clip(jax.random.uniform(keys[1], (BONDS, ORB, ORB, NX, NY, NZ), jnp.float32, -0.012, 0.012) * level_of(keys[1], (BONDS, ORB, ORB, NX, NY, NZ), ((3, 4), (4, 4), (5, 8)), -0.4, 0.0), -0.012, 0.012),
        "bond_open": set_ends((jax.random.randint(keys[2], (BONDS, NX, NY, NZ), 0, 4) < 3).astype(jnp.int32), jax.random.fold_in(keys[2], 1), 0, 1),
        "onsite_blocks": jnp.clip(jax.random.uniform(keys[3], (ORB, ORB, NX, NY, NZ), jnp.float32, -0.012, 0.012) * level_of(keys[3], (ORB, ORB, NX, NY, NZ), ((2, 4), (3, 4), (4, 8)), -0.4, 0.0), -0.012, 0.012),
        "orbital_levels": jnp.clip(jnp.exp(math.log(2.6) - 0.6931472 * jax.random.uniform(keys[4], (ORB, NX, NY, NZ), jnp.float32) ** level_of(keys[4], (ORB, NX, NY, NZ), ((1, 4), (2, 4), (3, 8)), -0.2, 0.2)), 1.3, 2.6),
        "column_shift": jnp.clip(jnp.exp(jax.random.uniform(keys[5], (COLS,), jnp.float32, math.log(0.05), math.log(1.0))), 0.05, 1.0),
    }


half_offsets = [(first, second, third) for first in (-1, 0, 1) for second in (-1, 0, 1) for third in (-1, 0, 1) if (first, second, third) > (0, 0, 0)]


def hop(blocks, vector):
    return jnp.einsum('ijxyz,xyzjc->xyzic', blocks.astype(jnp.float32), vector.astype(jnp.float32), precision=lax.Precision.HIGHEST)


def operate(vector, coupled, onsite_sym, atom_levels, column_shift):
    result = hop(onsite_sym, vector) + (atom_levels[..., None] + column_shift) * vector
    for bond_index, offset in enumerate(half_offsets):
        ahead = jnp.roll(vector, (-offset[0], -offset[1], -offset[2]), axis=(0, 1, 2))
        behind = jnp.roll(vector, offset, axis=(0, 1, 2))
        mirrored = jnp.roll(coupled[bond_index], offset, axis=(2, 3, 4))
        result = result + hop(coupled[bond_index], ahead) + hop(jnp.swapaxes(mirrored, 0, 1), behind)
    return result


def reference(right_side, bond_blocks, bond_open, onsite_blocks, orbital_levels, column_shift):
    coupled = bond_blocks * bond_open[:, None, None].astype(jnp.float32)
    onsite_sym = 0.5 * (onsite_blocks + jnp.swapaxes(onsite_blocks, 0, 1))
    atom_levels = jnp.transpose(orbital_levels, (1, 2, 3, 0))
    solution = jnp.zeros_like(right_side)
    residual = right_side
    direction = right_side
    norm_now = jnp.sum(residual * residual, axis=(0, 1, 2, 3))
    for iteration in range(ITERS):
        image = operate(direction, coupled, onsite_sym, atom_levels, column_shift)
        alpha = norm_now / jnp.sum(direction * image, axis=(0, 1, 2, 3))
        solution = solution + alpha * direction
        residual = residual - alpha * image
        norm_next = jnp.sum(residual * residual, axis=(0, 1, 2, 3))
        direction = residual + (norm_next / norm_now) * direction
        norm_now = norm_next
    return (solution, residual)
```

```python
import functools

import jax
import jax.numpy as jnp
from jax import lax
from jax.experimental import pallas as pl
from jax.experimental.pallas import tpu as pltpu
from jax.sharding import PartitionSpec as P

f32 = jnp.float32
bf16 = jnp.bfloat16

CENTRE = 1.95
GAMMA1 = 0.65 * 0.65 / 3.0
GAMMA2 = 0.65 * 0.65 * 4.0 / 15.0

half_offsets = [
    (first, second, third)
    for first in (-1, 0, 1)
    for second in (-1, 0, 1)
    for third in (-1, 0, 1)
    if (first, second, third) > (0, 0, 0)
]
directions = sorted(
    [
        (dx, dy, dz)
        for dx in (-1, 0, 1)
        for dy in (-1, 0, 1)
        for dz in (-1, 0, 1)
        if (dx, dy, dz) != (0, 0, 0)
    ],
    key=lambda d: (-abs(d[2]), abs(d[0]) + abs(d[1])),
)
AXES = ("gx", "gy", "gz")


def span_of(step, side):
    if step == 0:
        return slice(1, 5)
    if side == "source":
        return slice(4, 5) if step > 0 else slice(1, 2)
    return slice(0, 1) if step > 0 else slice(5, 6)


def kernel(
    sizes,
    right_ref,
    bond_ref,
    open_ref,
    onsite_ref,
    level_ref,
    shift_ref,
    sol_ref,
    res_ref,
    ext,
    last,
    diag,
    natural,
    flipped,
    stage1,
    stage2,
    stage3,
    from_x,
    from_y,
    from_z,
    matrix_t,
    matrix_hi,
    matrix_lo,
    sums,
    slots,
    load_sem,
    send_sem,
    recv_sem,
    coef_send,
    coef_recv,
    sum_send,
    sum_recv,
):
    me = [lax.axis_index(name) for name in AXES]

    def at(step):
        return tuple(lax.rem(me[n] + (step[n] + sizes[n]), sizes[n]) for n in range(3))

    def remote(source, target, send, recv, step):
        return pltpu.make_async_remote_copy(
            src_ref=source,
            dst_ref=target,
            send_sem=send,
            recv_sem=recv,
            device_id=at(step),
            device_id_type=pl.DeviceIdType.MESH,
        )

    sum_steps = (
        [(0, 0, n) for n in range(1, sizes[2])],
        [(0, n, 0) for n in range(1, sizes[1])],
        [(n, 0, 0) for n in range(1, sizes[0])],
    )
    peers = {tuple(d[n] % sizes[n] for n in range(3)) for d in directions}
    for steps in sum_steps:
        peers |= set(steps)
    peers = sorted(peers)

    load = pltpu.make_async_copy(right_ref, ext.at[0, 1:5, 1:5, 1:5], load_sem)
    load.start()
    barrier = pltpu.get_barrier_semaphore()
    for step in peers:
        pl.semaphore_signal(
            barrier, inc=1, device_id=at(step), device_id_type=pl.DeviceIdType.MESH
        )

    blocks = bond_ref[...] * open_ref[...].astype(f32)
    table = blocks.reshape(1024, 13).T
    for orb in range(4):
        natural[:, orb, :] = table[:, 256 * orb : 256 * orb + 256]
    table = jnp.swapaxes(blocks, 0, 1).reshape(1024, 13).T
    for orb in range(4):
        flipped[:, orb, :] = table[:, 256 * orb : 256 * orb + 256]

    pl.semaphore_wait(barrier, len(peers))

    waiting = []
    coef_x = remote(natural.at[4:13], from_x, coef_send.at[0], coef_recv.at[0], (1, 0, 0))
    coef_x.start()

    def exchange(number):
        copies = []
        for index, step in enumerate(directions):
            copy = remote(
                ext.at[(number,) + tuple(span_of(s, "source") for s in step)],
                ext.at[(number,) + tuple(span_of(s, "target") for s in step)],
                send_sem.at[number, index],
                recv_sem.at[number, index],
                step,
            )
            copy.start()
            copies.append(copy)
        return copies

    load.wait()
    copies = exchange(0)
    waiting += copies

    lane = lax.broadcasted_iota(jnp.int32, (4, 256), 1)
    place = ((lane >> 4) & 3, (lane >> 2) & 3, lane & 3)

    def moved(inner, outer, axis, step):
        stride = (16, 4, 1)[axis]
        if step > 0:
            mixed = jnp.where(place[axis] == 3, outer, inner)
            return jnp.where(
                place[axis] == 0,
                pltpu.roll(mixed, 256 - 3 * stride, 1),
                pltpu.roll(mixed, stride, 1),
            )
        mixed = jnp.where(place[axis] == 0, outer, inner)
        return jnp.where(
            place[axis] == 3,
            pltpu.roll(mixed, 3 * stride, 1),
            pltpu.roll(mixed, 256 - stride, 1),
        )

    coef_x.wait()
    for k in range(13):
        if k < 4:
            stage1[k] = natural[k]
        else:
            stage1[k] = moved(natural[k], from_x[k - 4], 0, 1)
    coef_y = [
        remote(stage1.at[1:4], from_y.at[0:3], coef_send.at[1], coef_recv.at[1], (0, 1, 0)),
        remote(stage1.at[10:13], from_y.at[3:6], coef_send.at[2], coef_recv.at[2], (0, 1, 0)),
        remote(stage1.at[4:7], from_y.at[6:9], coef_send.at[3], coef_recv.at[3], (0, -1, 0)),
    ]
    for copy in coef_y:
        copy.start()
    for copy in coef_y:
        copy.wait()
    slot_y = {1: 0, 2: 1, 3: 2, 10: 3, 11: 4, 12: 5, 4: 6, 5: 7, 6: 8}
    for k in range(13):
        if k in slot_y:
            stage2[k] = moved(stage1[k], from_y[slot_y[k]], 1, half_offsets[k][1])
        else:
            stage2[k] = stage1[k]
    order_z = [0, 3, 6, 9, 12, 1, 4, 7, 10]
    coef_z = []
    for index, k in enumerate(order_z):
        copy = remote(
            stage2.at[k],
            from_z.at[index],
            coef_send.at[4 + index],
            coef_recv.at[4 + index],
            (0, 0, half_offsets[k][2]),
        )
        copy.start()
        coef_z.append(copy)
    for copy in coef_z:
        copy.wait()
    for k in range(13):
        if k in order_z:
            stage3[k] = moved(stage2[k], from_z[order_z.index(k)], 2, half_offsets[k][2])
        else:
            stage3[k] = stage2[k]

    table = {(0, 0, 0): onsite_ref[...]}
    for k, offset in enumerate(half_offsets):
        table[offset] = flipped[k]
        table[tuple(-o for o in offset)] = stage3[k]
    for axis in range(3):
        kind = place[axis]
        kind = jnp.where(kind == 3, 0, kind)
        fresh = {}
        for key in table:
            cls = key[axis] % 3
            picks = []
            for residue in range(3):
                step = (cls - residue + 1) % 3 - 1
                picks.append(table[key[:axis] + (step,) + key[axis + 1 :]])
            fresh[key] = jnp.where(
                kind == 0, picks[0], jnp.where(kind == 1, picks[1], picks[2])
            )
        table = fresh
    near = [
        [(place[axis] >= e - 1) & (place[axis] <= e + 1) for e in range(-1, 5)]
        for axis in range(3)
    ]
    row = 0
    for ex in range(-1, 5):
        for ey in range(-1, 5):
            both = near[0][ex + 1] & near[1][ey + 1]
            for ez in range(-1, 5):
                key = tuple((e + 1) % 3 - 1 for e in (ex, ey, ez))
                matrix_t[row : row + 4, :] = jnp.where(both & near[2][ez + 1], table[key], 0.0)
                row += 4

    out_row = lax.broadcasted_iota(jnp.int32, (256, 256), 0)
    out_lane = lax.broadcasted_iota(jnp.int32, (256, 256), 1)
    same = ((out_row & 3) == (out_lane >> 6)) & ((out_row >> 2) == (out_lane & 63))
    pick = jnp.where(same, 1.0, 0.0).astype(bf16)
    entries = matrix_t[...]
    high = entries.astype(bf16)
    low = (entries - high.astype(f32)).astype(bf16)
    across = (((1,), (1,)), ((), ()))
    matrix_hi[...] = lax.dot_general(pick, high, across, preferred_element_type=f32).astype(bf16)
    matrix_lo[...] = lax.dot_general(pick, low, across, preferred_element_type=f32).astype(bf16)
    levels = jnp.sum(
        jnp.where(same, level_ref[...] - CENTRE, 0.0), axis=1, keepdims=True
    )
    diag[...] = jnp.broadcast_to(levels, (256, 256)).reshape(4, 4, 4, 4, 256)

    def core(number):
        return ext[number, 1:5, 1:5, 1:5]

    def applied(number):
        for copy in copies:
            copy.wait_recv()
        whole = ext[number].reshape(864, 256)
        high = whole.astype(bf16)
        low = (whole - high.astype(f32)).astype(bf16)
        total = (
            jnp.dot(matrix_hi[...], low, preferred_element_type=f32)
            + jnp.dot(matrix_lo[...], high, preferred_element_type=f32)
            + jnp.dot(matrix_hi[...], high, preferred_element_type=f32)
        )
        return total.reshape(4, 4, 4, 4, 256) + diag[...] * core(number)

    def product(left, right):
        return jnp.sum(jnp.sum(left * right, axis=(0, 1, 2)), axis=0, keepdims=True)

    ext[1, 1:5, 1:5, 1:5] = applied(0)
    copies = exchange(1)
    waiting += copies
    sums[0, 0:1] = product(core(0), core(0))
    sums[0, 1:2] = product(core(0), core(1))
    sums[0, 3:4] = product(core(1), core(1))
    ext[2, 1:5, 1:5, 1:5] = applied(1) - GAMMA1 * core(0)
    copies = exchange(2)
    waiting += copies
    sums[0, 2:3] = product(core(0), core(2))
    sums[0, 4:5] = product(core(1), core(2))
    sums[0, 5:6] = product(core(2), core(2))
    sums[0, 7:8] = jnp.zeros((1, 256), f32)
    last[...] = applied(2) - GAMMA2 * core(1)
    sums[0, 6:7] = product(core(2), last[...])

    base = 0
    for stage, steps in enumerate(sum_steps):
        sent = []
        for index, step in enumerate(steps):
            copy = remote(
                sums.at[stage],
                slots.at[base + index],
                sum_send.at[base + index],
                sum_recv.at[base + index],
                step,
            )
            copy.start()
            sent.append(copy)
        total = sums[stage]
        for index, copy in enumerate(sent):
            copy.wait_recv()
            total = total + slots[base + index]
        sums[stage + 1] = total
        waiting += sent
        base += len(steps)

    g00, g01, g02, g11, g12, g22, g23 = [sums[3, n : n + 1] for n in range(7)]
    theta = shift_ref[...] + CENTRE
    g03 = g12 - GAMMA2 * g01
    g13 = g22 + GAMMA1 * g02 - GAMMA2 * g11
    a0 = g00 / (theta * g00 + g01)
    s0 = a0
    r0, r1 = 1.0 - a0 * theta, -a0
    rr1 = r0 * r0 * g00 + 2.0 * r0 * r1 * g01 + r1 * r1 * g11
    p0, p1 = r0 + rr1 / g00, r1
    q0, q1, q2 = theta * p0 + GAMMA1 * p1, p0 + theta * p1, p1
    pq = p0 * (q0 * g00 + q1 * g01 + q2 * g02) + p1 * (q0 * g01 + q1 * g11 + q2 * g12)
    a1 = rr1 / pq
    s0, s1 = s0 + a1 * p0, a1 * p1
    r0, r1, r2 = r0 - a1 * q0, r1 - a1 * q1, -a1 * q2
    rr2 = (
        r0 * (r0 * g00 + r1 * g01 + r2 * g02)
        + r1 * (r0 * g01 + r1 * g11 + r2 * g12)
        + r2 * (r0 * g02 + r1 * g12 + r2 * g22)
    )
    ratio = rr2 / rr1
    p0, p1, p2 = r0 + ratio * p0, r1 + ratio * p1, r2
    q0 = theta * p0 + GAMMA1 * p1
    q1 = p0 + theta * p1 + GAMMA2 * p2
    q2 = p1 + theta * p2
    q3 = p2
    pq = (
        p0 * (q0 * g00 + q1 * g01 + q2 * g02 + q3 * g03)
        + p1 * (q0 * g01 + q1 * g11 + q2 * g12 + q3 * g13)
        + p2 * (q0 * g02 + q1 * g12 + q2 * g22 + q3 * g23)
    )
    a2 = rr2 / pq
    s0, s1, s2 = s0 + a2 * p0, s1 + a2 * p1, a2 * p2
    r0, r1, r2, r3 = r0 - a2 * q0, r1 - a2 * q1, r2 - a2 * q2, -a2 * q3
    sol_ref[...] = s0 * core(0) + s1 * core(1) + s2 * core(2)
    res_ref[...] = r0 * core(0) + r1 * core(1) + r2 * core(2) + r3 * last[...]
    for copy in waiting:
        copy.wait_send()


def solution(mesh):
    sizes = tuple(mesh.shape[name] for name in AXES)

    def per_device(right_side, bond_blocks, bond_open, onsite_blocks, orbital_levels, column_shift):
        onsite = (0.5 * (onsite_blocks + jnp.swapaxes(onsite_blocks, 0, 1))).reshape(4, 256)
        levels = orbital_levels.reshape(1, 256)
        bonds = jnp.transpose(bond_blocks, (1, 2, 3, 4, 5, 0))
        opened = jnp.transpose(bond_open, (1, 2, 3, 0))
        vmem = pl.BlockSpec(memory_space=pltpu.VMEM)
        shape = jax.ShapeDtypeStruct((4, 4, 4, 4, 256), f32)
        n_sums = sum(sizes) - 3
        return pl.pallas_call(
            functools.partial(kernel, sizes),
            out_shape=(shape, shape),
            in_specs=[pl.BlockSpec(memory_space=pl.ANY)] + [vmem] * 5,
            out_specs=(vmem, vmem),
            scratch_shapes=[
                pltpu.VMEM((3, 6, 6, 6, 4, 256), f32),
                pltpu.VMEM((4, 4, 4, 4, 256), f32),
                pltpu.VMEM((4, 4, 4, 4, 256), f32),
                pltpu.VMEM((13, 4, 256), f32),
                pltpu.VMEM((13, 4, 256), f32),
                pltpu.VMEM((13, 4, 256), f32),
                pltpu.VMEM((13, 4, 256), f32),
                pltpu.VMEM((13, 4, 256), f32),
                pltpu.VMEM((9, 4, 256), f32),
                pltpu.VMEM((9, 4, 256), f32),
                pltpu.VMEM((9, 4, 256), f32),
                pltpu.VMEM((864, 256), f32),
                pltpu.VMEM((256, 864), bf16),
                pltpu.VMEM((256, 864), bf16),
                pltpu.VMEM((4, 8, 256), f32),
                pltpu.VMEM((n_sums, 8, 256), f32),
                pltpu.SemaphoreType.DMA,
                pltpu.SemaphoreType.DMA((3, 26)),
                pltpu.SemaphoreType.DMA((3, 26)),
                pltpu.SemaphoreType.DMA((13,)),
                pltpu.SemaphoreType.DMA((13,)),
                pltpu.SemaphoreType.DMA((n_sums,)),
                pltpu.SemaphoreType.DMA((n_sums,)),
            ],
            compiler_params=pltpu.CompilerParams(collective_id=0, has_side_effects=True),
        )(right_side, bonds, opened, onsite, levels, column_shift.reshape(1, 256))

    return jax.shard_map(
        per_device,
        mesh=mesh,
        in_specs=(
            P("gx", "gy", "gz", None, None),
            P(None, None, None, "gx", "gy", "gz"),
            P(None, "gx", "gy", "gz"),
            P(None, None, "gx", "gy", "gz"),
            P(None, "gx", "gy", "gz"),
            P(),
        ),
        out_specs=(P("gx", "gy", "gz", None, None), P("gx", "gy", "gz", None, None)),
        check_vma=False,
    )
```

```python
import functools

import jax
import jax.numpy as jnp
from jax import lax
from jax.experimental import pallas as pl
from jax.experimental.pallas import tpu as pltpu
from jax.sharding import PartitionSpec as P

f32 = jnp.float32
bf16 = jnp.bfloat16
MESH = pl.DeviceIdType.MESH

CENTRE = 1.95
GAMMA1 = 0.65 * 0.65 / 3.0
GAMMA2 = 0.65 * 0.65 * 4.0 / 15.0
HALVES = 2
WIDTH = 256 // HALVES
AXES = ("gx", "gy", "gz")

ALL = (-1, 0, 1)
every = [(i, j, k) for i in ALL for j in ALL for k in ALL]
half_offsets = [o for o in every if o > (0, 0, 0)]
directions = sorted(
    [o for o in every if o != (0, 0, 0)],
    key=lambda d: (-abs(d[2]), abs(d[0]) + abs(d[1])),
)
hops = sorted(
    {
        tuple(o[n] * keep[n] for n in range(3))
        for o in half_offsets
        for keep in [(i, j, k) for i in (0, 1) for j in (0, 1) for k in (0, 1)]
    }
    - {(0, 0, 0)},
    key=lambda d: (-abs(d[2]), d),
)
cargo = {
    hop: [
        k
        for k, o in enumerate(half_offsets)
        if all(hop[n] in (0, o[n]) for n in range(3))
    ]
    for hop in hops
}
cargo_slot, cargo_start = {}, {}
for hop in hops:
    cargo_start[hop] = len(cargo_slot)
    for k in cargo[hop]:
        cargo_slot[hop, k] = len(cargo_slot)
CARGO = len(cargo_slot)

INSIDE = range(0, 4)
WITH_RIM = range(-1, 5)
groups = [
    (INSIDE, INSIDE, INSIDE),
    ((-1,), WITH_RIM, WITH_RIM),
    ((4,), WITH_RIM, WITH_RIM),
    (INSIDE, (-1,), WITH_RIM),
    (INSIDE, (4,), WITH_RIM),
    (INSIDE, INSIDE, (-1,)),
    (INSIDE, INSIDE, (4,)),
]


def span_of(step, side):
    if step == 0:
        return slice(1, 5)
    if side == "source":
        return slice(4, 5) if step > 0 else slice(1, 2)
    return slice(0, 1) if step > 0 else slice(5, 6)


def reach(values):
    return slice(values[0] + 1, values[-1] + 2)


def split(value):
    high = value.astype(bf16)
    return high, (value - high.astype(f32)).astype(bf16)


def coefficients(g00, g01, g02, g11, g12, g22, g23, theta):
    g03 = g12 - GAMMA2 * g01
    g13 = g22 + GAMMA1 * g02 - GAMMA2 * g11
    a0 = g00 / (theta * g00 + g01)
    s0 = a0
    r0, r1 = 1.0 - a0 * theta, -a0
    rr1 = r0 * r0 * g00 + 2.0 * r0 * r1 * g01 + r1 * r1 * g11
    p0, p1 = r0 + rr1 / g00, r1
    q0, q1, q2 = theta * p0 + GAMMA1 * p1, p0 + theta * p1, p1
    pq = p0 * (q0 * g00 + q1 * g01 + q2 * g02) + p1 * (q0 * g01 + q1 * g11 + q2 * g12)
    a1 = rr1 / pq
    s0, s1 = s0 + a1 * p0, a1 * p1
    r0, r1, r2 = r0 - a1 * q0, r1 - a1 * q1, -a1 * q2
    rr2 = (
        r0 * (r0 * g00 + r1 * g01 + r2 * g02)
        + r1 * (r0 * g01 + r1 * g11 + r2 * g12)
        + r2 * (r0 * g02 + r1 * g12 + r2 * g22)
    )
    ratio = rr2 / rr1
    p0, p1, p2 = r0 + ratio * p0, r1 + ratio * p1, r2
    q0 = theta * p0 + GAMMA1 * p1
    q1 = p0 + theta * p1 + GAMMA2 * p2
    q2 = p1 + theta * p2
    q3 = p2
    pq = (
        p0 * (q0 * g00 + q1 * g01 + q2 * g02 + q3 * g03)
        + p1 * (q0 * g01 + q1 * g11 + q2 * g12 + q3 * g13)
        + p2 * (q0 * g02 + q1 * g12 + q2 * g22 + q3 * g23)
    )
    a2 = rr2 / pq
    return (
        s0 + a2 * p0,
        s1 + a2 * p1,
        a2 * p2,
        r0 - a2 * q0,
        r1 - a2 * q1,
        r2 - a2 * q2,
        -a2 * q3,
    )


def kernel(
    sizes,
    right_ref,
    bond_ref,
    open_ref,
    onsite_ref,
    level_ref,
    shift_ref,
    first_ref,
    second_ref,
    third_ref,
    mix_ref,
    ext,
    last,
    partial,
    diag,
    bonds,
    opened,
    onsite,
    levels,
    natural,
    flipped,
    shifted,
    outgoing,
    incoming,
    matrix_t,
    matrix_hi,
    matrix_lo,
    sums,
    plane_slots,
    line_slots,
    final_sum,
    final_slots,
    load_sem,
    store_sem,
    halo_send,
    halo_recv,
    other_send,
    other_recv,
):
    me = [lax.axis_index(name) for name in AXES]

    def at(step):
        return tuple(lax.rem(me[n] + (step[n] + sizes[n]), sizes[n]) for n in range(3))

    def push(source, target, send, recv, step):
        pltpu.make_async_remote_copy(
            src_ref=source,
            dst_ref=target,
            send_sem=send,
            recv_sem=recv,
            device_id=at(step),
            device_id_type=MESH,
        ).start()

    def settle(like, sem):
        pltpu.make_async_copy(like, like, sem).wait()

    plane = [(i, j, 0) for i in range(sizes[0]) for j in range(sizes[1]) if (i, j) != (0, 0)]
    line = [(0, 0, k) for k in range(1, sizes[2])]
    others = [
        (i, j, k)
        for i in range(sizes[0])
        for j in range(sizes[1])
        for k in range(sizes[2])
        if (i, j, k) != (0, 0, 0)
    ]

    barrier = pltpu.get_barrier_semaphore()
    for step in others:
        pl.semaphore_signal(barrier, inc=1, device_id=at(step), device_id_type=MESH)
    loads = [
        pltpu.make_async_copy(bond_ref, bonds, load_sem.at[0]),
        pltpu.make_async_copy(open_ref, opened, load_sem.at[1]),
        pltpu.make_async_copy(onsite_ref, onsite, load_sem.at[2]),
        pltpu.make_async_copy(level_ref, levels, load_sem.at[3]),
    ]
    for half in range(HALVES):
        loads.append(
            pltpu.make_async_copy(
                right_ref.at[:, :, :, :, half * WIDTH : half * WIDTH + WIDTH],
                ext.at[0, half, 1:5, 1:5, 1:5],
                load_sem.at[4 + half],
            )
        )
    for copy in loads:
        copy.start()

    lane = lax.broadcasted_iota(jnp.int32, (4, 256), 1)
    place = ((lane >> 4) & 3, (lane >> 2) & 3, lane & 3)

    def cyclic(value, axis, step):
        stride = (16, 4, 1)[axis]
        if step == 0:
            return value
        if step > 0:
            return jnp.where(
                place[axis] == 0,
                pltpu.roll(value, 256 - 3 * stride, 1),
                pltpu.roll(value, stride, 1),
            )
        return jnp.where(
            place[axis] == 3,
            pltpu.roll(value, 3 * stride, 1),
            pltpu.roll(value, 256 - stride, 1),
        )

    with jax.named_scope("tables"):
        for copy in loads[:4]:
            copy.wait()
        blocks = bonds[...] * opened[...].astype(f32)
        table = blocks.reshape(1024, 13).T
        for orb in range(4):
            natural[:, orb, :] = table[:, 256 * orb : 256 * orb + 256]
        table = jnp.swapaxes(blocks, 0, 1).reshape(1024, 13).T
        for orb in range(4):
            flipped[:, orb, :] = table[:, 256 * orb : 256 * orb + 256]
        for k, offset in enumerate(half_offsets):
            value = natural[k]
            for axis in range(3):
                value = cyclic(value, axis, offset[axis])
            shifted[k] = value
            for hop in hops:
                if k in cargo[hop]:
                    outgoing[cargo_slot[hop, k]] = value

    with jax.named_scope("w_barrier"):
        pl.semaphore_wait(barrier, len(others))

    for hop in hops:
        rows = slice(cargo_start[hop], cargo_start[hop] + len(cargo[hop]))
        push(outgoing.at[rows], incoming.at[rows], other_send.at[0], other_recv.at[0], hop)

    def exchange(number, half):
        for step in directions:
            push(
                ext.at[(number, half) + tuple(span_of(s, "source") for s in step)],
                ext.at[(number, half) + tuple(span_of(s, "target") for s in step)],
                halo_send.at[number, half],
                halo_recv.at[number, half],
                step,
            )

    def halo_like(number, half):
        return matrix_t.at[0 : 152 * 4 * WIDTH // 256]

    for half in range(HALVES):
        loads[4 + half].wait()
        exchange(0, half)

    out_row = lax.broadcasted_iota(jnp.int32, (256, 256), 0)
    out_lane = lax.broadcasted_iota(jnp.int32, (256, 256), 1)
    same = ((out_row & 3) == (out_lane >> 6)) & ((out_row >> 2) == (out_lane & 63))
    pick = jnp.where(same, 1.0, 0.0).astype(bf16)

    with jax.named_scope("onsite"):
        spread = jnp.where(
            lax.broadcasted_iota(jnp.int32, (4, 256), 0) == (lane & 3), 1.0, 0.0
        )
        raw = onsite[...]
        raw = (0.5 * (raw + jnp.swapaxes(raw, 0, 1))).reshape(256, 4)
        wide = jnp.dot(
            raw, spread, precision=lax.Precision.HIGHEST, preferred_element_type=f32
        )
        keep = ((out_row >> 6) == (out_lane >> 6)) & (
            (out_row & 15) == ((out_lane >> 2) & 15)
        )
        wide = jnp.where(keep, wide, 0.0).reshape(4, 4, 16, 256)
        local = jnp.sum(jnp.sum(wide, axis=0), axis=1)
        wide = jnp.dot(
            levels[...].reshape(64, 4) - CENTRE,
            spread,
            precision=lax.Precision.HIGHEST,
            preferred_element_type=f32,
        )
        keep = out_row[0:64] == (out_lane[0:64] >> 2)
        level = jnp.sum(jnp.where(keep, wide, 0.0), axis=0, keepdims=True)
        level = jnp.sum(jnp.where(same, level, 0.0), axis=1, keepdims=True)
        diag[...] = jnp.broadcast_to(level, (256, WIDTH)).reshape(4, 4, 4, 4, WIDTH)

    near = [
        [(place[axis] >= e - 1) & (place[axis] <= e + 1) for e in WITH_RIM]
        for axis in range(3)
    ]

    def build(chosen, first_row, rows, behind):
        table = {(0, 0, 0): local}
        for k, offset in enumerate(half_offsets):
            table[offset] = flipped[k]
            table[tuple(-o for o in offset)] = behind(k, offset)
        for axis in range(3):
            kind = jnp.where(place[axis] == 3, 0, place[axis])
            fresh = {}
            for key in table:
                picks = []
                for residue in range(3):
                    step = (key[axis] % 3 - residue + 1) % 3 - 1
                    picks.append(table[key[:axis] + (step,) + key[axis + 1 :]])
                fresh[key] = jnp.where(
                    kind == 0, picks[0], jnp.where(kind == 1, picks[1], picks[2])
                )
            table = fresh
        row = first_row
        for group in chosen:
            for ex in group[0]:
                for ey in group[1]:
                    both = near[0][ex + 1] & near[1][ey + 1]
                    for ez in group[2]:
                        key = tuple((e + 1) % 3 - 1 for e in (ex, ey, ez))
                        matrix_t[row : row + 4, :] = jnp.where(
                            both & near[2][ez + 1], table[key], 0.0
                        )
                        row += 4
        across = (((1,), (1,)), ((), ()))
        span = slice(first_row, first_row + rows)
        high, low = split(matrix_t[span, :])
        matrix_hi[:, span] = lax.dot_general(
            pick, high, across, preferred_element_type=f32
        ).astype(bf16)
        matrix_lo[:, span] = lax.dot_general(
            pick, low, across, preferred_element_type=f32
        ).astype(bf16)

    def mirrored(k, offset):
        axes = [n for n in range(3) if offset[n]]

        def choose(position, hop):
            if position == len(axes):
                return incoming[cargo_slot[hop, k]] if any(hop) else shifted[k]
            axis = axes[position]
            edge = 0 if offset[axis] > 0 else 3
            away = hop[:axis] + (offset[axis],) + hop[axis + 1 :]
            return jnp.where(
                place[axis] == edge, choose(position + 1, away), choose(position + 1, hop)
            )

        return choose(0, (0, 0, 0))

    def times(span, value):
        high, low = split(value)
        return (
            jnp.dot(matrix_hi[:, span], low, preferred_element_type=f32)
            + jnp.dot(matrix_lo[:, span], high, preferred_element_type=f32)
            + jnp.dot(matrix_hi[:, span], high, preferred_element_type=f32)
        )

    def core(number, half):
        return ext[number, half, 1:5, 1:5, 1:5]

    def before(number, half):
        partial[half] = times(slice(0, 256), core(number, half).reshape(256, WIDTH))

    def after(number, half):
        with jax.named_scope("w_halo%d" % (2 * number + half)):
            settle(halo_like(number, half), halo_recv.at[number, half])
        rim = jnp.concatenate(
            [
                ext[(number, half) + tuple(reach(v) for v in group)].reshape(-1, WIDTH)
                for group in groups[1:]
            ],
            axis=0,
        )
        total = partial[half] + times(slice(256, 864), rim)
        return total.reshape(4, 4, 4, 4, WIDTH) + diag[...] * core(number, half)

    def product(left, right):
        return jnp.sum(jnp.sum(left * right, axis=(0, 1, 2)), axis=0, keepdims=True)

    stores = []

    def keep_copy(source, target, number, half):
        copy = pltpu.make_async_copy(
            source,
            target.at[:, :, :, :, half * WIDTH : half * WIDTH + WIDTH],
            store_sem.at[number, half],
        )
        copy.start()
        stores.append(copy)

    with jax.named_scope("inner"):
        build(groups[:1], 0, 256, lambda k, offset: shifted[k])
        for half in range(HALVES):
            before(0, half)
    with jax.named_scope("w_coef"):
        settle(incoming, other_recv.at[0])
    with jax.named_scope("rim"):
        build(groups[1:], 256, 608, mirrored)

    def lanes(half):
        return slice(half * WIDTH, half * WIDTH + WIDTH)

    for half in range(HALVES):
        ext[1, half, 1:5, 1:5, 1:5] = after(0, half)
        exchange(1, half)
        keep_copy(ext.at[1, half, 1:5, 1:5, 1:5], first_ref, 0, half)
        before(1, half)
        sums[0, 0, :, lanes(half)] = product(core(0, half), core(0, half))
        sums[0, 1, :, lanes(half)] = product(core(0, half), core(1, half))
        sums[0, 3, :, lanes(half)] = product(core(1, half), core(1, half))
    for half in range(HALVES):
        ext[2, half, 1:5, 1:5, 1:5] = after(1, half) - GAMMA1 * core(0, half)
        exchange(2, half)
        keep_copy(ext.at[2, half, 1:5, 1:5, 1:5], second_ref, 1, half)
        sums[0, 2, :, lanes(half)] = product(core(0, half), core(2, half))
        sums[0, 4, :, lanes(half)] = product(core(1, half), core(2, half))
        sums[0, 5, :, lanes(half)] = product(core(2, half), core(2, half))
    for index, step in enumerate(plane):
        push(sums.at[0], plane_slots.at[index], other_send.at[1], other_recv.at[1], step)
    for half in range(HALVES):
        before(2, half)
    with jax.named_scope("w_plane"):
        settle(plane_slots, other_recv.at[1])
    sums[1] = sums[0] + jnp.sum(plane_slots[...], axis=0)
    for index, step in enumerate(line):
        push(sums.at[1], line_slots.at[index], other_send.at[2], other_recv.at[2], step)
    for half in range(HALVES):
        last[half] = after(2, half) - GAMMA2 * core(1, half)
        final_sum[:, lanes(half)] = product(core(2, half), last[half])
        keep_copy(last.at[half], third_ref, 2, half)
    for index, step in enumerate(others):
        push(final_sum, final_slots.at[index], other_send.at[3], other_recv.at[3], step)
    with jax.named_scope("w_line"):
        settle(line_slots, other_recv.at[2])
    early = sums[1] + jnp.sum(line_slots[...], axis=0)
    with jax.named_scope("w_stores"):
        for copy in stores:
            copy.wait()
        for number in range(3):
            for half in range(HALVES):
                settle(halo_like(number, half), halo_send.at[number, half])
        settle(outgoing, other_send.at[0])
        settle(plane_slots, other_send.at[1])
        settle(line_slots, other_send.at[2])
    with jax.named_scope("w_final"):
        settle(final_slots, other_recv.at[3])
    g23 = final_sum[...] + jnp.sum(final_slots[...], axis=0)
    mix = coefficients(*[early[n] for n in range(6)], g23, shift_ref[...] + CENTRE)
    for n in range(7):
        mix_ref[n : n + 1, :] = mix[n]
    mix_ref[7:8, :] = jnp.zeros((1, 256), f32)
    settle(final_slots, other_send.at[3])


def solution(mesh):
    sizes = tuple(mesh.shape[name] for name in AXES)
    count = sizes[0] * sizes[1] * sizes[2]

    def per_device(right_side, bond_blocks, bond_open, onsite_blocks, orbital_levels, column_shift):
        vmem = pl.BlockSpec(memory_space=pltpu.VMEM)
        hbm = pl.BlockSpec(memory_space=pl.ANY)
        field = jax.ShapeDtypeStruct((4, 4, 4, 4, 256), f32)
        first, second, third, mix = pl.pallas_call(
            functools.partial(kernel, sizes),
            out_shape=(field, field, field, jax.ShapeDtypeStruct((8, 256), f32)),
            in_specs=[hbm] * 5 + [vmem],
            out_specs=(hbm, hbm, hbm, vmem),
            scratch_shapes=[
                pltpu.VMEM((3, HALVES, 6, 6, 6, 4, WIDTH), f32),
                pltpu.VMEM((HALVES, 4, 4, 4, 4, WIDTH), f32),
                pltpu.VMEM((HALVES, 256, WIDTH), f32),
                pltpu.VMEM((4, 4, 4, 4, WIDTH), f32),
                pltpu.VMEM((4, 4, 4, 4, 4, 13), f32),
                pltpu.VMEM((4, 4, 4, 13), jnp.int32),
                pltpu.VMEM((4, 4, 4, 4, 4), f32),
                pltpu.VMEM((4, 4, 4, 4), f32),
                pltpu.VMEM((13, 4, 256), f32),
                pltpu.VMEM((13, 4, 256), f32),
                pltpu.VMEM((13, 4, 256), f32),
                pltpu.VMEM((CARGO, 4, 256), f32),
                pltpu.VMEM((CARGO, 4, 256), f32),
                pltpu.VMEM((864, 256), f32),
                pltpu.VMEM((256, 864), bf16),
                pltpu.VMEM((256, 864), bf16),
                pltpu.VMEM((2, 6, 1, 256), f32),
                pltpu.VMEM((sizes[0] * sizes[1] - 1, 6, 1, 256), f32),
                pltpu.VMEM((sizes[2] - 1, 6, 1, 256), f32),
                pltpu.VMEM((1, 256), f32),
                pltpu.VMEM((count - 1, 1, 256), f32),
                pltpu.SemaphoreType.DMA((4 + HALVES,)),
                pltpu.SemaphoreType.DMA((3, HALVES)),
                pltpu.SemaphoreType.DMA((3, HALVES)),
                pltpu.SemaphoreType.DMA((3, HALVES)),
                pltpu.SemaphoreType.DMA((4,)),
                pltpu.SemaphoreType.DMA((4,)),
            ],
            compiler_params=pltpu.CompilerParams(collective_id=0, has_side_effects=True),
        )(
            right_side,
            jnp.transpose(bond_blocks, (1, 2, 3, 4, 5, 0)),
            jnp.transpose(bond_open, (1, 2, 3, 0)),
            onsite_blocks,
            orbital_levels,
            column_shift.reshape(1, 256),
        )
        answer = mix[0] * right_side + mix[1] * first + mix[2] * second
        left = mix[3] * right_side + mix[4] * first + mix[5] * second + mix[6] * third
        return answer, left

    return jax.shard_map(
        per_device,
        mesh=mesh,
        in_specs=(
            P("gx", "gy", "gz", None, None),
            P(None, None, None, "gx", "gy", "gz"),
            P(None, "gx", "gy", "gz"),
            P(None, None, "gx", "gy", "gz"),
            P(None, "gx", "gy", "gz"),
            P(),
        ),
        out_specs=(P("gx", "gy", "gz", None, None), P("gx", "gy", "gz", None, None)),
        check_vma=False,
    )
```

```python
import functools

import jax
import jax.numpy as jnp
from jax import lax
from jax.experimental import pallas as pl
from jax.experimental.pallas import tpu as pltpu
from jax.sharding import PartitionSpec as P

f32 = jnp.float32
bf16 = jnp.bfloat16
MESH = pl.DeviceIdType.MESH

CENTRE = 1.95
GAMMA1 = 0.65 * 0.65 / 3.0
GAMMA2 = 0.65 * 0.65 * 4.0 / 15.0
HALVES = 2
WIDTH = 256 // HALVES
AXES = ("gx", "gy", "gz")

ALL = (-1, 0, 1)
every = [(i, j, k) for i in ALL for j in ALL for k in ALL]
half_offsets = [o for o in every if o > (0, 0, 0)]
directions = sorted(
    [o for o in every if o != (0, 0, 0)],
    key=lambda d: (-abs(d[2]), abs(d[0]) + abs(d[1])),
)
hops = sorted(
    {
        tuple(o[n] * keep[n] for n in range(3))
        for o in half_offsets
        for keep in [(i, j, k) for i in (0, 1) for j in (0, 1) for k in (0, 1)]
    }
    - {(0, 0, 0)},
    key=lambda d: (-abs(d[2]), d),
)
cargo = {
    hop: [
        k
        for k, o in enumerate(half_offsets)
        if all(hop[n] in (0, o[n]) for n in range(3))
    ]
    for hop in hops
}
cargo_slot, slabs = {}, []
cargo_start = {}
for hop in hops:
    cargo_start[hop] = len(slabs)
    for index, k in enumerate(cargo[hop]):
        if index % 4 == 0:
            slabs.append((hop, []))
        slabs[-1][1].append(k)
        cargo_slot[hop, k] = (len(slabs) - 1, index % 4)
CARGO = len(slabs)

INSIDE = range(0, 4)
WITH_RIM = range(-1, 5)
groups = [
    (INSIDE, INSIDE, INSIDE),
    ((4,), WITH_RIM, INSIDE),
    ((-1,), WITH_RIM, INSIDE),
    (INSIDE, (-1,), INSIDE),
    (INSIDE, (4,), INSIDE),
    (WITH_RIM, WITH_RIM, (-1,)),
    (WITH_RIM, WITH_RIM, (4,)),
]


def span_of(step, side):
    if step == 0:
        return slice(1, 5)
    if side == "source":
        return slice(4, 5) if step > 0 else slice(1, 2)
    return slice(0, 1) if step > 0 else slice(5, 6)


def reach(values):
    return slice(values[0] + 1, values[-1] + 2)


def split(value):
    high = value.astype(bf16)
    return high, (value - high.astype(f32)).astype(bf16)


def early_part(g00, g01, g02, g11, g12, g22, theta):
    g03 = g12 - GAMMA2 * g01
    g13 = g22 + GAMMA1 * g02 - GAMMA2 * g11
    a0 = g00 / (theta * g00 + g01)
    s0 = a0
    r0, r1 = 1.0 - a0 * theta, -a0
    rr1 = r0 * r0 * g00 + 2.0 * r0 * r1 * g01 + r1 * r1 * g11
    p0, p1 = r0 + rr1 / g00, r1
    q0, q1, q2 = theta * p0 + GAMMA1 * p1, p0 + theta * p1, p1
    pq = p0 * (q0 * g00 + q1 * g01 + q2 * g02) + p1 * (q0 * g01 + q1 * g11 + q2 * g12)
    a1 = rr1 / pq
    s0, s1 = s0 + a1 * p0, a1 * p1
    r0, r1, r2 = r0 - a1 * q0, r1 - a1 * q1, -a1 * q2
    rr2 = (
        r0 * (r0 * g00 + r1 * g01 + r2 * g02)
        + r1 * (r0 * g01 + r1 * g11 + r2 * g12)
        + r2 * (r0 * g02 + r1 * g12 + r2 * g22)
    )
    ratio = rr2 / rr1
    p0, p1, p2 = r0 + ratio * p0, r1 + ratio * p1, r2
    q0 = theta * p0 + GAMMA1 * p1
    q1 = p0 + theta * p1 + GAMMA2 * p2
    q2 = p1 + theta * p2
    q3 = p2
    pq = (
        p0 * (q0 * g00 + q1 * g01 + q2 * g02 + q3 * g03)
        + p1 * (q0 * g01 + q1 * g11 + q2 * g12 + q3 * g13)
        + p2 * (q0 * g02 + q1 * g12 + q2 * g22)
    )
    return rr2, pq, p2 * q3, (s0, s1, 0.0, r0, r1, r2, 0.0), (p0, p1, p2, -q0, -q1, -q2, -q3)


def kernel(
    sizes,
    right_ref,
    bond_ref,
    open_ref,
    onsite_ref,
    level_ref,
    shift_ref,
    zeroth_ref,
    first_ref,
    second_ref,
    third_ref,
    mix_ref,
    ext,
    last,
    partial,
    diag,
    bonds,
    opened,
    onsite,
    levels,
    natural,
    flipped,
    shifted,
    outgoing,
    incoming,
    matrix_t,
    matrix_hi,
    matrix_lo,
    first_sum,
    first_plane,
    first_line,
    sums,
    plane_slots,
    line_slots,
    final_sum,
    final_slots,
    load_sem,
    store_sem,
    halo_send,
    halo_recv,
    other_send,
    other_recv,
    final_send,
    final_recv,
):
    me = [lax.axis_index(name) for name in AXES]

    def at(step):
        return tuple(lax.rem(me[n] + (step[n] + sizes[n]), sizes[n]) for n in range(3))

    def push(source, target, send, recv, step):
        pltpu.make_async_remote_copy(
            src_ref=source,
            dst_ref=target,
            send_sem=send,
            recv_sem=recv,
            device_id=at(step),
            device_id_type=MESH,
        ).start()

    def settle(like, sem):
        pltpu.make_async_copy(like, like, sem).wait()

    plane = [(i, j, 0) for i in range(sizes[0]) for j in range(sizes[1]) if (i, j) != (0, 0)]
    line = [(0, 0, k) for k in range(1, sizes[2])]
    others = [
        (i, j, k)
        for i in range(sizes[0])
        for j in range(sizes[1])
        for k in range(sizes[2])
        if (i, j, k) != (0, 0, 0)
    ]

    greeted = {tuple(d[n] % sizes[n] for n in range(3)) for d in directions}
    greeted = sorted(greeted | set(plane) | set(line))

    loads = []
    for half in range(HALVES):
        loads.append(
            pltpu.make_async_copy(
                right_ref.at[:, :, :, :, half * WIDTH : half * WIDTH + WIDTH],
                ext.at[0, half, 1:5, 1:5, 1:5],
                load_sem.at[half],
            )
        )
    tables = [
        pltpu.make_async_copy(bond_ref, bonds, load_sem.at[HALVES]),
        pltpu.make_async_copy(open_ref, opened, load_sem.at[HALVES + 1]),
        pltpu.make_async_copy(onsite_ref, onsite, load_sem.at[HALVES + 2]),
        pltpu.make_async_copy(level_ref, levels, load_sem.at[HALVES + 3]),
    ]
    for copy in tables + loads:
        copy.start()
    barrier = pltpu.get_barrier_semaphore()
    with jax.named_scope("greet"):
        for step in greeted:
            pl.semaphore_signal(barrier, inc=1, device_id=at(step), device_id_type=MESH)

    lane = lax.broadcasted_iota(jnp.int32, (4, 256), 1)
    place = ((lane >> 4) & 3, (lane >> 2) & 3, lane & 3)

    def cyclic(value, axis, step):
        stride = (16, 4, 1)[axis]
        if step == 0:
            return value
        if step > 0:
            return jnp.where(
                place[axis] == 0,
                pltpu.roll(value, 256 - 3 * stride, 1),
                pltpu.roll(value, stride, 1),
            )
        return jnp.where(
            place[axis] == 3,
            pltpu.roll(value, 3 * stride, 1),
            pltpu.roll(value, 256 - stride, 1),
        )

    def layer(hop):
        axis = [n for n in range(3) if hop[n]][0]
        return axis, (16, 4, 1)[axis], 0 if hop[axis] > 0 else 3

    def packed(hop, values):
        axis, stride, edge = layer(hop)
        total = values[0]
        for index in range(1, len(values)):
            spot = (edge + index) % 4
            moved = pltpu.roll(values[index], (stride * (spot - edge)) % 256, 1)
            total = jnp.where(place[axis] == spot, moved, total)
        return total

    def unpacked(hop, k):
        axis, stride, edge = layer(hop)
        slot, index = cargo_slot[hop, k]
        spot = (edge + index) % 4
        value = incoming[slot]
        return value if index == 0 else pltpu.roll(value, (stride * (edge - spot)) % 256, 1)

    with jax.named_scope("tables"):
        for copy in tables:
            copy.wait()
        blocks = bonds[...] * opened[...].astype(f32)
        table = blocks.reshape(1024, 13).T
        for orb in range(4):
            natural[:, orb, :] = table[:, 256 * orb : 256 * orb + 256]
        table = jnp.swapaxes(blocks, 0, 1).reshape(1024, 13).T
        for orb in range(4):
            flipped[:, orb, :] = table[:, 256 * orb : 256 * orb + 256]
        for k, offset in enumerate(half_offsets):
            value = natural[k]
            for axis in range(3):
                value = cyclic(value, axis, offset[axis])
            shifted[k] = value
        for slot, (hop, blocks) in enumerate(slabs):
            outgoing[slot] = packed(hop, [shifted[k] for k in blocks])

    def exchange(number, half):
        for step in directions:
            part = 1 if step[2] else 0
            push(
                ext.at[(number, half) + tuple(span_of(s, "source") for s in step)],
                ext.at[(number, half) + tuple(span_of(s, "target") for s in step)],
                halo_send.at[number, half],
                halo_recv.at[number, half, part],
                step,
            )

    def halo_like(part):
        return matrix_t.at[0 : (80, 72, 152)[part] * 4 * WIDTH // 256]

    with jax.named_scope("w_barrier"):
        pl.semaphore_wait(barrier, len(greeted))
    for hop in hops:
        count = sum(1 for slab in slabs if slab[0] == hop)
        rows = slice(cargo_start[hop], cargo_start[hop] + count)
        push(outgoing.at[rows], incoming.at[rows], other_send.at[0], other_recv.at[0], hop)
    for half in range(HALVES):
        loads[half].wait()
        exchange(0, half)

    out_row = lax.broadcasted_iota(jnp.int32, (256, 256), 0)
    out_lane = lax.broadcasted_iota(jnp.int32, (256, 256), 1)
    same = ((out_row & 3) == (out_lane >> 6)) & ((out_row >> 2) == (out_lane & 63))
    pick = jnp.where(same, 1.0, 0.0).astype(bf16)

    with jax.named_scope("onsite"):
        spread = jnp.where(
            lax.broadcasted_iota(jnp.int32, (4, 256), 0) == (lane & 3), 1.0, 0.0
        )
        raw = onsite[...]
        raw = (0.5 * (raw + jnp.swapaxes(raw, 0, 1))).reshape(256, 4)
        wide = jnp.dot(
            raw, spread, precision=lax.Precision.HIGHEST, preferred_element_type=f32
        )
        keep = ((out_row >> 6) == (out_lane >> 6)) & (
            (out_row & 15) == ((out_lane >> 2) & 15)
        )
        wide = jnp.where(keep, wide, 0.0).reshape(4, 4, 16, 256)
        local = jnp.sum(jnp.sum(wide, axis=0), axis=1)
        wide = jnp.dot(
            levels[...].reshape(64, 4) - CENTRE,
            spread,
            precision=lax.Precision.HIGHEST,
            preferred_element_type=f32,
        )
        keep = out_row[0:64] == (out_lane[0:64] >> 2)
        level = jnp.sum(jnp.where(keep, wide, 0.0), axis=0, keepdims=True)
        level = jnp.sum(jnp.where(same, level, 0.0), axis=1, keepdims=True)
        diag[...] = jnp.broadcast_to(level, (256, WIDTH)).reshape(4, 4, 4, 4, WIDTH)

    near = [
        [(place[axis] >= e - 1) & (place[axis] <= e + 1) for e in WITH_RIM]
        for axis in range(3)
    ]

    def build(chosen, first_row, rows, behind):
        table = {(0, 0, 0): local}
        for k, offset in enumerate(half_offsets):
            table[offset] = flipped[k]
            table[tuple(-o for o in offset)] = behind(k, offset)
        for axis in range(3):
            kind = jnp.where(place[axis] == 3, 0, place[axis])
            fresh = {}
            for key in table:
                picks = []
                for residue in range(3):
                    step = (key[axis] % 3 - residue + 1) % 3 - 1
                    picks.append(table[key[:axis] + (step,) + key[axis + 1 :]])
                fresh[key] = jnp.where(
                    kind == 0, picks[0], jnp.where(kind == 1, picks[1], picks[2])
                )
            table = fresh
        row = first_row
        for group in chosen:
            for ex in group[0]:
                for ey in group[1]:
                    both = near[0][ex + 1] & near[1][ey + 1]
                    for ez in group[2]:
                        key = tuple((e + 1) % 3 - 1 for e in (ex, ey, ez))
                        matrix_t[row : row + 4, :] = jnp.where(
                            both & near[2][ez + 1], table[key], 0.0
                        )
                        row += 4
        across = (((1,), (1,)), ((), ()))
        span = slice(first_row, first_row + rows)
        high, low = split(matrix_t[span, :])
        matrix_hi[:, span] = lax.dot_general(
            pick, high, across, preferred_element_type=f32
        ).astype(bf16)
        matrix_lo[:, span] = lax.dot_general(
            pick, low, across, preferred_element_type=f32
        ).astype(bf16)

    def mirrored(k, offset):
        axes = [n for n in range(3) if offset[n]]

        def choose(position, hop):
            if position == len(axes):
                return unpacked(hop, k) if any(hop) else shifted[k]
            axis = axes[position]
            edge = 0 if offset[axis] > 0 else 3
            away = hop[:axis] + (offset[axis],) + hop[axis + 1 :]
            return jnp.where(
                place[axis] == edge, choose(position + 1, away), choose(position + 1, hop)
            )

        return choose(0, (0, 0, 0))

    def times(span, value):
        high, low = split(value)
        return (
            jnp.dot(matrix_hi[:, span], low, preferred_element_type=f32)
            + jnp.dot(matrix_lo[:, span], high, preferred_element_type=f32)
            + jnp.dot(matrix_hi[:, span], high, preferred_element_type=f32)
        )

    def core(number, half):
        return ext[number, half, 1:5, 1:5, 1:5]

    def before(number, half):
        partial[half] = times(slice(0, 256), core(number, half).reshape(256, WIDTH))

    def rim_times(number, half, part):
        with jax.named_scope("w_halo%d_%d" % (2 * number + half, part)):
            settle(halo_like(part), halo_recv.at[number, half, part])
        rim = jnp.concatenate(
            [
                ext[(number, half) + tuple(reach(v) for v in group)].reshape(-1, WIDTH)
                for group in (groups[1:5], groups[5:7])[part]
            ],
            axis=0,
        )
        return times((slice(256, 576), slice(576, 864))[part], rim)

    def after(number, half):
        partial[half] = (partial[half] + rim_times(number, half, 0)) + (
            diag[...] * core(number, half)
        ).reshape(256, WIDTH)
        total = partial[half] + rim_times(number, half, 1)
        return total.reshape(4, 4, 4, 4, WIDTH)

    def product(left, right):
        return jnp.sum(jnp.sum(left * right, axis=(0, 1, 2)), axis=0, keepdims=True)

    stores = []

    def keep_copy(source, target, number, half):
        copy = pltpu.make_async_copy(
            source,
            target.at[:, :, :, :, half * WIDTH : half * WIDTH + WIDTH],
            store_sem.at[number, half],
        )
        copy.start()
        stores.append(copy)

    def lanes(half):
        return slice(half * WIDTH, half * WIDTH + WIDTH)

    own = (first_sum, sums)
    from_plane = (first_plane, plane_slots)
    along_line = (first_line, line_slots)

    def to_plane(group):
        for index, step in enumerate(plane):
            push(
                own[group].at[0],
                from_plane[group].at[index],
                other_send.at[1 + group],
                other_recv.at[1 + group],
                step,
            )

    def to_line(group):
        with jax.named_scope("w_plane%d" % group):
            settle(from_plane[group], other_recv.at[1 + group])
        own[group][1] = own[group][0] + jnp.sum(from_plane[group][...], axis=0)
        for index, step in enumerate(line):
            push(
                own[group].at[1],
                along_line[group].at[index],
                other_send.at[3 + group],
                other_recv.at[3 + group],
                step,
            )

    def from_line(group):
        with jax.named_scope("w_line%d" % group):
            settle(along_line[group], other_recv.at[3 + group])
        return own[group][1] + jnp.sum(along_line[group][...], axis=0)

    for half in range(HALVES):
        keep_copy(ext.at[0, half, 1:5, 1:5, 1:5], zeroth_ref, 0, half)
    with jax.named_scope("inner"):
        build(groups[:2], 0, 352, lambda k, offset: shifted[k])
        for half in range(HALVES):
            before(0, half)
    for half in range(HALVES):
        first_sum[0, :, :, lanes(half)] = product(core(0, half), core(0, half))[None]
    to_plane(0)
    with jax.named_scope("w_coef"):
        settle(incoming, other_recv.at[0])
    with jax.named_scope("rim"):
        build(groups[2:], 352, 512, mirrored)

    for half in range(HALVES):
        ext[1, half, 1:5, 1:5, 1:5] = after(0, half)
        exchange(1, half)
        keep_copy(ext.at[1, half, 1:5, 1:5, 1:5], first_ref, 1, half)
        before(1, half)
        if half == 0:
            to_line(0)
        sums[0, 0, :, lanes(half)] = product(core(0, half), core(1, half))
        sums[0, 1, :, lanes(half)] = product(core(1, half), core(1, half))
    for half in range(HALVES):
        ext[2, half, 1:5, 1:5, 1:5] = after(1, half) - GAMMA1 * core(0, half)
        exchange(2, half)
        keep_copy(ext.at[2, half, 1:5, 1:5, 1:5], second_ref, 2, half)
        before(2, half)
        sums[0, 2, :, lanes(half)] = product(core(0, half), core(2, half))
        sums[0, 3, :, lanes(half)] = product(core(1, half), core(2, half))
        sums[0, 4, :, lanes(half)] = product(core(2, half), core(2, half))
    to_plane(1)
    g00 = from_line(0)[0]
    for half in range(HALVES):
        last[half] = after(2, half) - GAMMA2 * core(1, half)
        final_sum[half] = product(core(2, half), last[half])
        for index, step in enumerate(others):
            push(
                final_sum.at[half],
                final_slots.at[half, index],
                final_send.at[half],
                final_recv.at[half],
                step,
            )
        keep_copy(last.at[half], third_ref, 3, half)
    to_line(1)
    rest = from_line(1)
    rr2, pq, weight, start, along = early_part(
        g00, rest[0], rest[2], rest[1], rest[3], rest[4], shift_ref[...] + CENTRE
    )
    with jax.named_scope("w_stores"):
        for copy in stores:
            copy.wait()
        for number in range(3):
            for half in range(HALVES):
                settle(halo_like(2), halo_send.at[number, half])
        settle(outgoing, other_send.at[0])
        for group in range(2):
            settle(from_plane[group], other_send.at[1 + group])
            settle(along_line[group], other_send.at[3 + group])
    totals = []
    for half in range(HALVES):
        with jax.named_scope("w_final%d" % half):
            settle(final_slots.at[half], final_recv.at[half])
        totals.append(final_sum[half] + jnp.sum(final_slots[half], axis=0))
    a2 = rr2 / (pq + weight * jnp.concatenate(totals, axis=1))
    for n in range(7):
        mix_ref[n : n + 1, :] = start[n] + a2 * along[n]
    for half in range(HALVES):
        settle(final_slots.at[half], final_send.at[half])


def combine(zeroth_ref, first_ref, second_ref, third_ref, mix_ref, sol_ref, res_ref, sol, res, sem):
    copies = []
    for x in range(4):
        zeroth, first, second = zeroth_ref[x], first_ref[x], second_ref[x]
        sol[x] = mix_ref[0] * zeroth + mix_ref[1] * first + mix_ref[2] * second
        res[x] = (
            mix_ref[3] * zeroth
            + mix_ref[4] * first
            + mix_ref[5] * second
            + mix_ref[6] * third_ref[x]
        )
        copies.append(pltpu.make_async_copy(sol.at[x], sol_ref.at[x], sem.at[0, x]))
        copies.append(pltpu.make_async_copy(res.at[x], res_ref.at[x], sem.at[1, x]))
        for copy in copies[-2:]:
            copy.start()
    for copy in copies:
        copy.wait()


def solution(mesh):
    sizes = tuple(mesh.shape[name] for name in AXES)
    count = sizes[0] * sizes[1] * sizes[2]

    def per_device(right_side, bond_blocks, bond_open, onsite_blocks, orbital_levels, column_shift):
        vmem = pl.BlockSpec(memory_space=pltpu.VMEM)
        hbm = pl.BlockSpec(memory_space=pl.ANY)
        out = jax.ShapeDtypeStruct((4, 4, 4, 4, 256), f32)
        field = pltpu.VMEM((4, 4, 4, 4, 256), f32)
        kept = pl.pallas_call(
            functools.partial(kernel, sizes),
            out_shape=(field,) * 4 + (pltpu.VMEM((7, 256), f32),),
            in_specs=[hbm] * 5 + [vmem],
            out_specs=(hbm,) * 4 + (vmem,),
            scratch_shapes=[
                pltpu.VMEM((3, HALVES, 6, 6, 6, 4, WIDTH), f32),
                pltpu.VMEM((HALVES, 4, 4, 4, 4, WIDTH), f32),
                pltpu.VMEM((HALVES, 256, WIDTH), f32),
                pltpu.VMEM((4, 4, 4, 4, WIDTH), f32),
                pltpu.VMEM((4, 4, 4, 4, 4, 13), f32),
                pltpu.VMEM((4, 4, 4, 13), jnp.int32),
                pltpu.VMEM((4, 4, 4, 4, 4), f32),
                pltpu.VMEM((4, 4, 4, 4), f32),
                pltpu.VMEM((13, 4, 256), f32),
                pltpu.VMEM((13, 4, 256), f32),
                pltpu.VMEM((13, 4, 256), f32),
                pltpu.VMEM((CARGO, 4, 256), f32),
                pltpu.VMEM((CARGO, 4, 256), f32),
                pltpu.VMEM((864, 256), f32),
                pltpu.VMEM((256, 864), bf16),
                pltpu.VMEM((256, 864), bf16),
                pltpu.VMEM((2, 1, 1, 256), f32),
                pltpu.VMEM((sizes[0] * sizes[1] - 1, 1, 1, 256), f32),
                pltpu.VMEM((sizes[2] - 1, 1, 1, 256), f32),
                pltpu.VMEM((2, 5, 1, 256), f32),
                pltpu.VMEM((sizes[0] * sizes[1] - 1, 5, 1, 256), f32),
                pltpu.VMEM((sizes[2] - 1, 5, 1, 256), f32),
                pltpu.VMEM((HALVES, 1, WIDTH), f32),
                pltpu.VMEM((HALVES, count - 1, 1, WIDTH), f32),
                pltpu.SemaphoreType.DMA((4 + HALVES,)),
                pltpu.SemaphoreType.DMA((4, HALVES)),
                pltpu.SemaphoreType.DMA((3, HALVES)),
                pltpu.SemaphoreType.DMA((3, HALVES, 2)),
                pltpu.SemaphoreType.DMA((5,)),
                pltpu.SemaphoreType.DMA((5,)),
                pltpu.SemaphoreType.DMA((HALVES,)),
                pltpu.SemaphoreType.DMA((HALVES,)),
            ],
            compiler_params=pltpu.CompilerParams(collective_id=0, has_side_effects=True),
        )(
            right_side,
            jnp.transpose(bond_blocks, (1, 2, 3, 4, 5, 0)),
            jnp.transpose(bond_open, (1, 2, 3, 0)),
            onsite_blocks,
            orbital_levels,
            column_shift.reshape(1, 256),
        )
        return pl.pallas_call(
            combine,
            out_shape=(out, out),
            in_specs=[vmem] * 5,
            out_specs=(hbm, hbm),
            scratch_shapes=[
                pltpu.VMEM((4, 4, 4, 4, 256), f32),
                pltpu.VMEM((4, 4, 4, 4, 256), f32),
                pltpu.SemaphoreType.DMA((2, 4)),
            ],
        )(*[pltpu.with_memory_space_constraint(value, pltpu.VMEM) for value in kept])

    return jax.shard_map(
        per_device,
        mesh=mesh,
        in_specs=(
            P("gx", "gy", "gz", None, None),
            P(None, None, None, "gx", "gy", "gz"),
            P(None, "gx", "gy", "gz"),
            P(None, None, "gx", "gy", "gz"),
            P(None, "gx", "gy", "gz"),
            P(),
        ),
        out_specs=(P("gx", "gy", "gz", None, None), P("gx", "gy", "gz", None, None)),
        check_vma=False,
    )
```

```python
import functools

import jax
import jax.numpy as jnp
from jax import lax
from jax.experimental import pallas as pl
from jax.experimental.pallas import tpu as pltpu
from jax.sharding import PartitionSpec as P

f32 = jnp.float32
bf16 = jnp.bfloat16
MESH = pl.DeviceIdType.MESH

CENTRE = 1.95
GAMMA1 = 0.65 * 0.65 / 3.0
GAMMA2 = 0.65 * 0.65 * 4.0 / 15.0
HALVES = 2
WIDTH = 256 // HALVES
AXES = ("gx", "gy", "gz")

ALL = (-1, 0, 1)
every = [(i, j, k) for i in ALL for j in ALL for k in ALL]
half_offsets = [o for o in every if o > (0, 0, 0)]
directions = sorted(
    [o for o in every if o != (0, 0, 0)],
    key=lambda d: (-abs(d[2]), abs(d[0]) + abs(d[1])),
)
hops = sorted(
    {
        tuple(o[n] * keep[n] for n in range(3))
        for o in half_offsets
        for keep in [(i, j, k) for i in (0, 1) for j in (0, 1) for k in (0, 1)]
    }
    - {(0, 0, 0)},
    key=lambda d: (-abs(d[2]), d),
)
cargo = {
    hop: [
        k
        for k, o in enumerate(half_offsets)
        if all(hop[n] in (0, o[n]) for n in range(3))
    ]
    for hop in hops
}
cargo_slot, slabs = {}, []
cargo_start = {}
for hop in hops:
    cargo_start[hop] = len(slabs)
    for index, k in enumerate(cargo[hop]):
        if index % 4 == 0:
            slabs.append((hop, []))
        slabs[-1][1].append(k)
        cargo_slot[hop, k] = (len(slabs) - 1, index % 4)
CARGO = len(slabs)

INSIDE = range(0, 4)
WITH_RIM = range(-1, 5)
groups = [
    (INSIDE, INSIDE, INSIDE),
    ((4,), WITH_RIM, INSIDE),
    ((-1,), WITH_RIM, INSIDE),
    (INSIDE, (-1,), INSIDE),
    (INSIDE, (4,), INSIDE),
    (WITH_RIM, WITH_RIM, (-1,)),
    (WITH_RIM, WITH_RIM, (4,)),
]


def span_of(step, side):
    if step == 0:
        return slice(1, 5)
    if side == "source":
        return slice(4, 5) if step > 0 else slice(1, 2)
    return slice(0, 1) if step > 0 else slice(5, 6)


def reach(values):
    return slice(values[0] + 1, values[-1] + 2)


def split(value):
    high = value.astype(bf16)
    return high, (value - high.astype(f32)).astype(bf16)


def early_part(g00, g01, g02, g11, g12, g22, theta):
    g03 = g12 - GAMMA2 * g01
    g13 = g22 + GAMMA1 * g02 - GAMMA2 * g11
    a0 = g00 / (theta * g00 + g01)
    s0 = a0
    r0, r1 = 1.0 - a0 * theta, -a0
    rr1 = r0 * r0 * g00 + 2.0 * r0 * r1 * g01 + r1 * r1 * g11
    p0, p1 = r0 + rr1 / g00, r1
    q0, q1, q2 = theta * p0 + GAMMA1 * p1, p0 + theta * p1, p1
    pq = p0 * (q0 * g00 + q1 * g01 + q2 * g02) + p1 * (q0 * g01 + q1 * g11 + q2 * g12)
    a1 = rr1 / pq
    s0, s1 = s0 + a1 * p0, a1 * p1
    r0, r1, r2 = r0 - a1 * q0, r1 - a1 * q1, -a1 * q2
    rr2 = (
        r0 * (r0 * g00 + r1 * g01 + r2 * g02)
        + r1 * (r0 * g01 + r1 * g11 + r2 * g12)
        + r2 * (r0 * g02 + r1 * g12 + r2 * g22)
    )
    ratio = rr2 / rr1
    p0, p1, p2 = r0 + ratio * p0, r1 + ratio * p1, r2
    q0 = theta * p0 + GAMMA1 * p1
    q1 = p0 + theta * p1 + GAMMA2 * p2
    q2 = p1 + theta * p2
    q3 = p2
    pq = (
        p0 * (q0 * g00 + q1 * g01 + q2 * g02 + q3 * g03)
        + p1 * (q0 * g01 + q1 * g11 + q2 * g12 + q3 * g13)
        + p2 * (q0 * g02 + q1 * g12 + q2 * g22)
    )
    return rr2, pq, p2 * q3, (s0, s1, 0.0, r0, r1, r2, 0.0), (p0, p1, p2, -q0, -q1, -q2, -q3)


def kernel(
    sizes,
    right_ref,
    bond_ref,
    open_ref,
    onsite_ref,
    level_ref,
    shift_ref,
    zeroth_ref,
    first_ref,
    second_ref,
    third_ref,
    mix_ref,
    ext,
    last,
    partial,
    diag,
    bonds,
    opened,
    onsite,
    levels,
    shift,
    natural,
    flipped,
    shifted,
    outgoing,
    incoming,
    matrix_t,
    matrix_hi,
    matrix_lo,
    first_sum,
    first_plane,
    first_line,
    sums,
    plane_slots,
    line_slots,
    final_sum,
    final_slots,
    load_sem,
    store_sem,
    halo_send,
    halo_recv,
    other_send,
    other_recv,
    final_recv,
):
    me = [lax.axis_index(name) for name in AXES]

    def at(step):
        return tuple(lax.rem(me[n] + (step[n] + sizes[n]), sizes[n]) for n in range(3))

    def push(source, target, send, recv, step):
        pltpu.make_async_remote_copy(
            src_ref=source,
            dst_ref=target,
            send_sem=send,
            recv_sem=recv,
            device_id=at(step),
            device_id_type=MESH,
        ).start()

    def settle(like, sem):
        pltpu.make_async_copy(like, like, sem).wait()

    plane = [(i, j, 0) for i in range(sizes[0]) for j in range(sizes[1]) if (i, j) != (0, 0)]
    line = [(0, 0, k) for k in range(1, sizes[2])]
    others = [
        (i, j, k)
        for i in range(sizes[0])
        for j in range(sizes[1])
        for k in range(sizes[2])
        if (i, j, k) != (0, 0, 0)
    ]
    far = {0: 0, 1: 3, 2: 4, 3: 3, 4: 2}
    others.sort(
        key=lambda d: -(min(d[1], sizes[1] - d[1]) + far.get(min(d[2], sizes[2] - d[2]), 4))
    )

    greeted = {tuple(d[n] % sizes[n] for n in range(3)) for d in directions}
    greeted = sorted(greeted | set(plane) | set(line))

    loads = []
    for half in range(HALVES):
        loads.append(
            pltpu.make_async_copy(
                right_ref.at[:, :, :, :, half * WIDTH : half * WIDTH + WIDTH],
                ext.at[0, half, 1:5, 1:5, 1:5],
                store_sem.at[half],
            )
        )
    tables = [
        pltpu.make_async_copy(bond_ref, bonds, load_sem.at[0]),
        pltpu.make_async_copy(open_ref, opened, load_sem.at[1]),
        pltpu.make_async_copy(onsite_ref, onsite, load_sem.at[2]),
        pltpu.make_async_copy(level_ref, levels, load_sem.at[3]),
        pltpu.make_async_copy(shift_ref, shift, load_sem.at[4]),
    ]
    for copy in tables + loads:
        copy.start()
    barrier = pltpu.get_barrier_semaphore()
    with jax.named_scope("greet"):
        for step in greeted:
            pl.semaphore_signal(barrier, inc=1, device_id=at(step), device_id_type=MESH)

    lane = lax.broadcasted_iota(jnp.int32, (4, 256), 1)
    place = ((lane >> 4) & 3, (lane >> 2) & 3, lane & 3)

    def cyclic(value, axis, step):
        stride = (16, 4, 1)[axis]
        if step == 0:
            return value
        if step > 0:
            return jnp.where(
                place[axis] == 0,
                pltpu.roll(value, 256 - 3 * stride, 1),
                pltpu.roll(value, stride, 1),
            )
        return jnp.where(
            place[axis] == 3,
            pltpu.roll(value, 3 * stride, 1),
            pltpu.roll(value, 256 - stride, 1),
        )

    def layer(hop):
        axis = [n for n in range(3) if hop[n]][0]
        return axis, (16, 4, 1)[axis], 0 if hop[axis] > 0 else 3

    def packed(hop, values):
        axis, stride, edge = layer(hop)
        total = values[0]
        for index in range(1, len(values)):
            spot = (edge + index) % 4
            moved = pltpu.roll(values[index], (stride * (spot - edge)) % 256, 1)
            total = jnp.where(place[axis] == spot, moved, total)
        return total

    def unpacked(hop, k):
        axis, stride, edge = layer(hop)
        slot, index = cargo_slot[hop, k]
        spot = (edge + index) % 4
        value = incoming[slot]
        return value if index == 0 else pltpu.roll(value, (stride * (edge - spot)) % 256, 1)

    with jax.named_scope("tables"):
        for copy in tables:
            copy.wait()
        blocks = bonds[...] * opened[...].astype(f32)
        table = blocks.reshape(1024, 13).T
        for orb in range(4):
            natural[:, orb, :] = table[:, 256 * orb : 256 * orb + 256]
        table = jnp.swapaxes(blocks, 0, 1).reshape(1024, 13).T
        for orb in range(4):
            flipped[:, orb, :] = table[:, 256 * orb : 256 * orb + 256]
        for k, offset in enumerate(half_offsets):
            value = natural[k]
            for axis in range(3):
                value = cyclic(value, axis, offset[axis])
            shifted[k] = value
        for slot, (hop, blocks) in enumerate(slabs):
            outgoing[slot] = packed(hop, [shifted[k] for k in blocks])

    def exchange(number, half):
        if number:
            settle(halo_like(2), halo_send.at[half])
        for step in directions:
            part = 1 if step[2] else 0
            push(
                ext.at[(number, half) + tuple(span_of(s, "source") for s in step)],
                ext.at[(number, half) + tuple(span_of(s, "target") for s in step)],
                halo_send.at[half],
                halo_recv.at[number % 2, half, part],
                step,
            )

    def halo_like(part):
        return matrix_t.at[0 : (80, 72, 152)[part] * 4 * WIDTH // 256]

    with jax.named_scope("w_barrier"):
        pl.semaphore_wait(barrier, len(greeted))
    for hop in hops:
        count = sum(1 for slab in slabs if slab[0] == hop)
        rows = slice(cargo_start[hop], cargo_start[hop] + count)
        push(outgoing.at[rows], incoming.at[rows], other_send.at[0], other_recv.at[0], hop)
    for half in range(HALVES):
        loads[half].wait()
        exchange(0, half)

    out_row = lax.broadcasted_iota(jnp.int32, (256, 256), 0)
    out_lane = lax.broadcasted_iota(jnp.int32, (256, 256), 1)
    same = ((out_row & 3) == (out_lane >> 6)) & ((out_row >> 2) == (out_lane & 63))
    pick = jnp.where(same, 1.0, 0.0).astype(bf16)

    with jax.named_scope("onsite"):
        spread = jnp.where(
            lax.broadcasted_iota(jnp.int32, (4, 256), 0) == (lane & 3), 1.0, 0.0
        )
        raw = onsite[...]
        raw = (0.5 * (raw + jnp.swapaxes(raw, 0, 1))).reshape(256, 4)
        wide = jnp.dot(
            raw, spread, precision=lax.Precision.HIGHEST, preferred_element_type=f32
        )
        keep = ((out_row >> 6) == (out_lane >> 6)) & (
            (out_row & 15) == ((out_lane >> 2) & 15)
        )
        wide = jnp.where(keep, wide, 0.0).reshape(4, 4, 16, 256)
        local = jnp.sum(jnp.sum(wide, axis=0), axis=1)
        wide = jnp.dot(
            levels[...].reshape(64, 4) - CENTRE,
            spread,
            precision=lax.Precision.HIGHEST,
            preferred_element_type=f32,
        )
        keep = out_row[0:64] == (out_lane[0:64] >> 2)
        level = jnp.sum(jnp.where(keep, wide, 0.0), axis=0, keepdims=True)
        level = jnp.sum(jnp.where(same, level, 0.0), axis=1, keepdims=True)
        diag[...] = jnp.broadcast_to(level, (256, WIDTH)).reshape(4, 4, 4, 4, WIDTH)

    near = [
        [(place[axis] >= e - 1) & (place[axis] <= e + 1) for e in WITH_RIM]
        for axis in range(3)
    ]

    def build(chosen, first_row, rows, behind):
        table = {(0, 0, 0): local}
        for k, offset in enumerate(half_offsets):
            table[offset] = flipped[k]
            table[tuple(-o for o in offset)] = behind(k, offset)
        for axis in range(3):
            kind = jnp.where(place[axis] == 3, 0, place[axis])
            fresh = {}
            for key in table:
                picks = []
                for residue in range(3):
                    step = (key[axis] % 3 - residue + 1) % 3 - 1
                    picks.append(table[key[:axis] + (step,) + key[axis + 1 :]])
                fresh[key] = jnp.where(
                    kind == 0, picks[0], jnp.where(kind == 1, picks[1], picks[2])
                )
            table = fresh
        row = first_row
        for group in chosen:
            for ex in group[0]:
                for ey in group[1]:
                    both = near[0][ex + 1] & near[1][ey + 1]
                    for ez in group[2]:
                        key = tuple((e + 1) % 3 - 1 for e in (ex, ey, ez))
                        matrix_t[row : row + 4, :] = jnp.where(
                            both & near[2][ez + 1], table[key], 0.0
                        )
                        row += 4
        across = (((1,), (1,)), ((), ()))
        span = slice(first_row, first_row + rows)
        high, low = split(matrix_t[span, :])
        matrix_hi[:, span] = lax.dot_general(
            pick, high, across, preferred_element_type=f32
        ).astype(bf16)
        matrix_lo[:, span] = lax.dot_general(
            pick, low, across, preferred_element_type=f32
        ).astype(bf16)

    def mirrored(k, offset):
        axes = [n for n in range(3) if offset[n]]

        def choose(position, hop):
            if position == len(axes):
                return unpacked(hop, k) if any(hop) else shifted[k]
            axis = axes[position]
            edge = 0 if offset[axis] > 0 else 3
            away = hop[:axis] + (offset[axis],) + hop[axis + 1 :]
            return jnp.where(
                place[axis] == edge, choose(position + 1, away), choose(position + 1, hop)
            )

        return choose(0, (0, 0, 0))

    def times(span, value):
        high, low = split(value)
        return (
            jnp.dot(matrix_hi[:, span], low, preferred_element_type=f32)
            + jnp.dot(matrix_lo[:, span], high, preferred_element_type=f32)
            + jnp.dot(matrix_hi[:, span], high, preferred_element_type=f32)
        )

    def core(number, half):
        return ext[number, half, 1:5, 1:5, 1:5]

    def before(number, half):
        partial[half] = times(slice(0, 256), core(number, half).reshape(256, WIDTH))

    def rim_times(number, half, part):
        with jax.named_scope("w_halo%d_%d" % (2 * number + half, part)):
            settle(halo_like(part), halo_recv.at[number % 2, half, part])
        rim = jnp.concatenate(
            [
                ext[(number, half) + tuple(reach(v) for v in group)].reshape(-1, WIDTH)
                for group in (groups[1:5], groups[5:7])[part]
            ],
            axis=0,
        )
        return times((slice(256, 576), slice(576, 864))[part], rim)

    def after(number, half, line_between=False):
        partial[half] = (partial[half] + rim_times(number, half, 0)) + (
            diag[...] * core(number, half)
        ).reshape(256, WIDTH)
        if line_between:
            to_line(1)
        total = partial[half] + rim_times(number, half, 1)
        return total.reshape(4, 4, 4, 4, WIDTH)

    def product(left, right):
        return jnp.sum(jnp.sum(left * right, axis=(0, 1, 2)), axis=0, keepdims=True)

    stores = [None] * HALVES

    def keep_copy(source, target, number, half):
        if number:
            stores[half].wait()
        copy = pltpu.make_async_copy(
            source,
            target.at[:, :, :, :, half * WIDTH : half * WIDTH + WIDTH],
            store_sem.at[half],
        )
        copy.start()
        stores[half] = copy

    def lanes(half):
        return slice(half * WIDTH, half * WIDTH + WIDTH)

    own = (first_sum, sums)
    from_plane = (first_plane, plane_slots)
    along_line = (first_line, line_slots)

    def to_plane(group):
        settle(along_line[0] if group else outgoing, other_send.at[0])
        for index, step in enumerate(plane):
            push(
                own[group].at[0],
                from_plane[group].at[index],
                other_send.at[0],
                other_recv.at[1 + group],
                step,
            )

    def to_line(group):
        with jax.named_scope("w_plane%d" % group):
            settle(from_plane[group], other_recv.at[1 + group])
        own[group][1] = own[group][0] + jnp.sum(from_plane[group][...], axis=0)
        settle(from_plane[group], other_send.at[0])
        for index, step in enumerate(line):
            push(
                own[group].at[1],
                along_line[group].at[index],
                other_send.at[0],
                other_recv.at[3 + group],
                step,
            )

    def from_line(group):
        with jax.named_scope("w_line%d" % group):
            settle(along_line[group], other_recv.at[3 + group])
        return own[group][1] + jnp.sum(along_line[group][...], axis=0)

    for half in range(HALVES):
        keep_copy(ext.at[0, half, 1:5, 1:5, 1:5], zeroth_ref, 0, half)
    with jax.named_scope("inner"):
        build(groups[:2], 0, 352, lambda k, offset: shifted[k])
        for half in range(HALVES):
            before(0, half)
    for half in range(HALVES):
        first_sum[0, :, :, lanes(half)] = product(core(0, half), core(0, half))[None]
    to_plane(0)
    with jax.named_scope("w_coef"):
        settle(incoming, other_recv.at[0])
    with jax.named_scope("rim"):
        build(groups[2:], 352, 512, mirrored)

    for half in range(HALVES):
        ext[1, half, 1:5, 1:5, 1:5] = after(0, half)
        exchange(1, half)
        keep_copy(ext.at[1, half, 1:5, 1:5, 1:5], first_ref, 1, half)
        before(1, half)
        if half == 0:
            to_line(0)
        sums[0, 0, :, lanes(half)] = product(core(0, half), core(1, half))
        sums[0, 1, :, lanes(half)] = product(core(1, half), core(1, half))
    for half in range(HALVES):
        ext[2, half, 1:5, 1:5, 1:5] = after(1, half) - GAMMA1 * core(0, half)
        exchange(2, half)
        keep_copy(ext.at[2, half, 1:5, 1:5, 1:5], second_ref, 2, half)
        before(2, half)
        sums[0, 2, :, lanes(half)] = product(core(0, half), core(2, half))
        sums[0, 3, :, lanes(half)] = product(core(1, half), core(2, half))
        sums[0, 4, :, lanes(half)] = product(core(2, half), core(2, half))
    to_plane(1)
    g00 = from_line(0)[0]
    for half in range(HALVES):
        last[half] = after(2, half, half == HALVES - 1) - GAMMA2 * core(1, half)
        final_sum[half] = product(core(2, half), last[half])
        settle(halo_like(2), halo_send.at[half])
        for index, step in enumerate(others):
            push(
                final_sum.at[half],
                final_slots.at[half, index],
                halo_send.at[half],
                final_recv.at[half],
                step,
            )
        keep_copy(last.at[half], third_ref, 3, half)
    rest = from_line(1)
    rr2, pq, weight, start, along = early_part(
        g00, rest[0], rest[2], rest[1], rest[3], rest[4], shift[...] + CENTRE
    )
    with jax.named_scope("w_stores"):
        for copy in stores:
            copy.wait()
        settle(along_line[1], other_send.at[0])
    totals = []
    for half in range(HALVES):
        with jax.named_scope("w_final%d" % half):
            settle(final_slots.at[half], final_recv.at[half])
        totals.append(final_sum[half] + jnp.sum(final_slots[half], axis=0))
    a2 = rr2 / (pq + weight * jnp.concatenate(totals, axis=1))
    for n in range(7):
        mix_ref[n : n + 1, :] = start[n] + a2 * along[n]
    for half in range(HALVES):
        settle(final_slots.at[half], halo_send.at[half])


def combine(zeroth_ref, first_ref, second_ref, third_ref, mix_ref, sol_ref, res_ref, sol, res, sem):
    copies = []
    for x in range(4):
        zeroth, first, second = zeroth_ref[x], first_ref[x], second_ref[x]
        sol[x] = mix_ref[0] * zeroth + mix_ref[1] * first + mix_ref[2] * second
        res[x] = (
            mix_ref[3] * zeroth
            + mix_ref[4] * first
            + mix_ref[5] * second
            + mix_ref[6] * third_ref[x]
        )
        copies.append(pltpu.make_async_copy(sol.at[x], sol_ref.at[x], sem.at[0, x]))
        copies.append(pltpu.make_async_copy(res.at[x], res_ref.at[x], sem.at[1, x]))
        for copy in copies[-2:]:
            copy.start()
    for copy in copies:
        copy.wait()


def solution(mesh):
    sizes = tuple(mesh.shape[name] for name in AXES)
    count = sizes[0] * sizes[1] * sizes[2]

    def per_device(right_side, bond_blocks, bond_open, onsite_blocks, orbital_levels, column_shift):
        vmem = pl.BlockSpec(memory_space=pltpu.VMEM)
        hbm = pl.BlockSpec(memory_space=pl.ANY)
        out = jax.ShapeDtypeStruct((4, 4, 4, 4, 256), f32)
        field = pltpu.VMEM((4, 4, 4, 4, 256), f32)
        kept = pl.pallas_call(
            functools.partial(kernel, sizes),
            out_shape=(field,) * 4 + (pltpu.VMEM((7, 256), f32),),
            in_specs=[hbm] * 6,
            out_specs=(hbm,) * 4 + (vmem,),
            scratch_shapes=[
                pltpu.VMEM((3, HALVES, 6, 6, 6, 4, WIDTH), f32),
                pltpu.VMEM((HALVES, 4, 4, 4, 4, WIDTH), f32),
                pltpu.VMEM((HALVES, 256, WIDTH), f32),
                pltpu.VMEM((4, 4, 4, 4, WIDTH), f32),
                pltpu.VMEM((4, 4, 4, 4, 4, 13), f32),
                pltpu.VMEM((4, 4, 4, 13), jnp.int32),
                pltpu.VMEM((4, 4, 4, 4, 4), f32),
                pltpu.VMEM((4, 4, 4, 4), f32),
                pltpu.VMEM((1, 256), f32),
                pltpu.VMEM((13, 4, 256), f32),
                pltpu.VMEM((13, 4, 256), f32),
                pltpu.VMEM((13, 4, 256), f32),
                pltpu.VMEM((CARGO, 4, 256), f32),
                pltpu.VMEM((CARGO, 4, 256), f32),
                pltpu.VMEM((864, 256), f32),
                pltpu.VMEM((256, 864), bf16),
                pltpu.VMEM((256, 864), bf16),
                pltpu.VMEM((2, 1, 1, 256), f32),
                pltpu.VMEM((sizes[0] * sizes[1] - 1, 1, 1, 256), f32),
                pltpu.VMEM((sizes[2] - 1, 1, 1, 256), f32),
                pltpu.VMEM((2, 5, 1, 256), f32),
                pltpu.VMEM((sizes[0] * sizes[1] - 1, 5, 1, 256), f32),
                pltpu.VMEM((sizes[2] - 1, 5, 1, 256), f32),
                pltpu.VMEM((HALVES, 1, WIDTH), f32),
                pltpu.VMEM((HALVES, count - 1, 1, WIDTH), f32),
                pltpu.SemaphoreType.DMA((5,)),
                pltpu.SemaphoreType.DMA((HALVES,)),
                pltpu.SemaphoreType.DMA((HALVES,)),
                pltpu.SemaphoreType.DMA((2, HALVES, 2)),
                pltpu.SemaphoreType.DMA((1,)),
                pltpu.SemaphoreType.DMA((5,)),
                pltpu.SemaphoreType.DMA((HALVES,)),
            ],
            compiler_params=pltpu.CompilerParams(collective_id=0, has_side_effects=True),
        )(
            right_side,
            jnp.transpose(bond_blocks, (1, 2, 3, 4, 5, 0)),
            jnp.transpose(bond_open, (1, 2, 3, 0)),
            onsite_blocks,
            orbital_levels,
            column_shift.reshape(1, 256),
        )
        return pl.pallas_call(
            combine,
            out_shape=(out, out),
            in_specs=[vmem] * 5,
            out_specs=(hbm, hbm),
            scratch_shapes=[
                pltpu.VMEM((4, 4, 4, 4, 256), f32),
                pltpu.VMEM((4, 4, 4, 4, 256), f32),
                pltpu.SemaphoreType.DMA((2, 4)),
            ],
        )(*[pltpu.with_memory_space_constraint(value, pltpu.VMEM) for value in kept])

    return jax.shard_map(
        per_device,
        mesh=mesh,
        in_specs=(
            P("gx", "gy", "gz", None, None),
            P(None, None, None, "gx", "gy", "gz"),
            P(None, "gx", "gy", "gz"),
            P(None, None, "gx", "gy", "gz"),
            P(None, "gx", "gy", "gz"),
            P(),
        ),
        out_specs=(P("gx", "gy", "gz", None, None), P("gx", "gy", "gz", None, None)),
        check_vma=False,
    )
```

```python
import functools

import jax
import jax.numpy as jnp
from jax import lax
from jax.experimental import pallas as pl
from jax.experimental.pallas import tpu as pltpu
from jax.sharding import PartitionSpec as P

f32 = jnp.float32
bf16 = jnp.bfloat16
MESH = pl.DeviceIdType.MESH

CENTRE = 1.95
GAMMA1 = 0.65 * 0.65 / 3.0
GAMMA2 = 0.65 * 0.65 * 4.0 / 15.0
HALVES = 2
WIDTH = 256 // HALVES
AXES = ("gx", "gy", "gz")

ALL = (-1, 0, 1)
every = [(i, j, k) for i in ALL for j in ALL for k in ALL]
half_offsets = [o for o in every if o > (0, 0, 0)]
directions = sorted(
    [o for o in every if o != (0, 0, 0)],
    key=lambda d: (-abs(d[2]), abs(d[0]) + abs(d[1])),
)
hops = sorted(
    {
        tuple(o[n] * keep[n] for n in range(3))
        for o in half_offsets
        for keep in [(i, j, k) for i in (0, 1) for j in (0, 1) for k in (0, 1)]
    }
    - {(0, 0, 0)},
    key=lambda d: (-abs(d[2]), d),
)
cargo = {
    hop: [
        k
        for k, o in enumerate(half_offsets)
        if all(hop[n] in (0, o[n]) for n in range(3))
    ]
    for hop in hops
}
cargo_slot, slabs = {}, []
cargo_start = {}
for hop in hops:
    cargo_start[hop] = len(slabs)
    for index, k in enumerate(cargo[hop]):
        if index % 4 == 0:
            slabs.append((hop, []))
        slabs[-1][1].append(k)
        cargo_slot[hop, k] = (len(slabs) - 1, index % 4)
CARGO = len(slabs)

INSIDE = range(0, 4)
WITH_RIM = range(-1, 5)
groups = [
    (INSIDE, INSIDE, INSIDE),
    ((4,), WITH_RIM, INSIDE),
    ((-1,), WITH_RIM, INSIDE),
    (INSIDE, (-1,), INSIDE),
    (INSIDE, (4,), INSIDE),
    (WITH_RIM, WITH_RIM, (-1,)),
    (WITH_RIM, WITH_RIM, (4,)),
]


def span_of(step, side):
    if step == 0:
        return slice(1, 5)
    if side == "source":
        return slice(4, 5) if step > 0 else slice(1, 2)
    return slice(0, 1) if step > 0 else slice(5, 6)


def reach(values):
    return slice(values[0] + 1, values[-1] + 2)


def split(value):
    high = value.astype(bf16)
    return high, (value - high.astype(f32)).astype(bf16)


def early_part(g00, g01, g02, g11, g12, g22, theta):
    g03 = g12 - GAMMA2 * g01
    g13 = g22 + GAMMA1 * g02 - GAMMA2 * g11
    a0 = g00 / (theta * g00 + g01)
    s0 = a0
    r0, r1 = 1.0 - a0 * theta, -a0
    rr1 = r0 * r0 * g00 + 2.0 * r0 * r1 * g01 + r1 * r1 * g11
    p0, p1 = r0 + rr1 / g00, r1
    q0, q1, q2 = theta * p0 + GAMMA1 * p1, p0 + theta * p1, p1
    pq = p0 * (q0 * g00 + q1 * g01 + q2 * g02) + p1 * (q0 * g01 + q1 * g11 + q2 * g12)
    a1 = rr1 / pq
    s0, s1 = s0 + a1 * p0, a1 * p1
    r0, r1, r2 = r0 - a1 * q0, r1 - a1 * q1, -a1 * q2
    rr2 = (
        r0 * (r0 * g00 + r1 * g01 + r2 * g02)
        + r1 * (r0 * g01 + r1 * g11 + r2 * g12)
        + r2 * (r0 * g02 + r1 * g12 + r2 * g22)
    )
    ratio = rr2 / rr1
    p0, p1, p2 = r0 + ratio * p0, r1 + ratio * p1, r2
    q0 = theta * p0 + GAMMA1 * p1
    q1 = p0 + theta * p1 + GAMMA2 * p2
    q2 = p1 + theta * p2
    q3 = p2
    pq = (
        p0 * (q0 * g00 + q1 * g01 + q2 * g02 + q3 * g03)
        + p1 * (q0 * g01 + q1 * g11 + q2 * g12 + q3 * g13)
        + p2 * (q0 * g02 + q1 * g12 + q2 * g22)
    )
    return rr2, pq, p2 * q3, (s0, s1, 0.0, r0, r1, r2, 0.0), (p0, p1, p2, -q0, -q1, -q2, -q3)


def kernel(
    sizes,
    right_ref,
    bond_ref,
    open_ref,
    onsite_ref,
    level_ref,
    shift_ref,
    zeroth_ref,
    first_ref,
    second_ref,
    third_ref,
    mix_ref,
    ext,
    last,
    partial,
    diag,
    bonds,
    opened,
    onsite,
    levels,
    shift,
    natural,
    flipped,
    shifted,
    outgoing,
    incoming,
    matrix_t,
    matrix_hi,
    matrix_lo,
    matrix_z,
    first_sum,
    first_plane,
    first_line,
    sums,
    plane_slots,
    line_slots,
    final_sum,
    final_slots,
    load_sem,
    store_sem,
    halo_send,
    halo_recv,
    other_send,
    other_recv,
    final_recv,
):
    me = [lax.axis_index(name) for name in AXES]

    def at(step):
        return tuple(lax.rem(me[n] + (step[n] + sizes[n]), sizes[n]) for n in range(3))

    def push(source, target, send, recv, step):
        pltpu.make_async_remote_copy(
            src_ref=source,
            dst_ref=target,
            send_sem=send,
            recv_sem=recv,
            device_id=at(step),
            device_id_type=MESH,
        ).start()

    def settle(like, sem):
        pltpu.make_async_copy(like, like, sem).wait()

    plane = [(i, j, 0) for i in range(sizes[0]) for j in range(sizes[1]) if (i, j) != (0, 0)]
    line = [(0, 0, k) for k in range(1, sizes[2])]
    others = [
        (i, j, k)
        for i in range(sizes[0])
        for j in range(sizes[1])
        for k in range(sizes[2])
        if (i, j, k) != (0, 0, 0)
    ]
    far = {0: 0, 1: 3, 2: 4, 3: 3, 4: 2}

    def path(step):
        return -(min(step[1], sizes[1] - step[1]) + far.get(min(step[2], sizes[2] - step[2]), 4))

    others.sort(key=path)
    greeted = {tuple(d[n] % sizes[n] for n in range(3)) for d in directions}
    greeted = sorted(greeted | set(plane) | set(line), key=lambda d: (path(d), d))


    loads = []
    for half in range(HALVES):
        loads.append(
            pltpu.make_async_copy(
                right_ref.at[:, :, :, :, half * WIDTH : half * WIDTH + WIDTH],
                ext.at[0, half, 1:5, 1:5, 1:5],
                store_sem.at[half],
            )
        )
    tables = [
        pltpu.make_async_copy(bond_ref, bonds, load_sem.at[0]),
        pltpu.make_async_copy(open_ref, opened, load_sem.at[1]),
        pltpu.make_async_copy(onsite_ref, onsite, load_sem.at[2]),
        pltpu.make_async_copy(level_ref, levels, load_sem.at[3]),
        pltpu.make_async_copy(shift_ref, shift, load_sem.at[4]),
    ]
    for copy in tables + loads:
        copy.start()
    barrier = pltpu.get_barrier_semaphore()
    with jax.named_scope("greet"):
        for step in greeted:
            pl.semaphore_signal(barrier, inc=1, device_id=at(step), device_id_type=MESH)

    lane = lax.broadcasted_iota(jnp.int32, (4, 256), 1)
    place = ((lane >> 4) & 3, (lane >> 2) & 3, lane & 3)

    def cyclic(value, axis, step):
        stride = (16, 4, 1)[axis]
        if step == 0:
            return value
        if step > 0:
            return jnp.where(
                place[axis] == 0,
                pltpu.roll(value, 256 - 3 * stride, 1),
                pltpu.roll(value, stride, 1),
            )
        return jnp.where(
            place[axis] == 3,
            pltpu.roll(value, 3 * stride, 1),
            pltpu.roll(value, 256 - stride, 1),
        )

    def layer(hop):
        axis = [n for n in range(3) if hop[n]][0]
        return axis, (16, 4, 1)[axis], 0 if hop[axis] > 0 else 3

    def packed(hop, values):
        axis, stride, edge = layer(hop)
        total = values[0]
        for index in range(1, len(values)):
            spot = (edge + index) % 4
            moved = pltpu.roll(values[index], (stride * (spot - edge)) % 256, 1)
            total = jnp.where(place[axis] == spot, moved, total)
        return total

    def unpacked(hop, k):
        axis, stride, edge = layer(hop)
        slot, index = cargo_slot[hop, k]
        spot = (edge + index) % 4
        value = incoming[slot]
        return value if index == 0 else pltpu.roll(value, (stride * (edge - spot)) % 256, 1)

    with jax.named_scope("tables"):
        for copy in tables:
            copy.wait()
        blocks = bonds[...] * opened[...].astype(f32)
        table = blocks.reshape(1024, 13).T
        for orb in range(4):
            natural[:, orb, :] = table[:, 256 * orb : 256 * orb + 256]
        table = jnp.swapaxes(blocks, 0, 1).reshape(1024, 13).T
        for orb in range(4):
            flipped[:, orb, :] = table[:, 256 * orb : 256 * orb + 256]
        for k, offset in enumerate(half_offsets):
            value = natural[k]
            for axis in range(3):
                value = cyclic(value, axis, offset[axis])
            shifted[k] = value
        for slot, (hop, blocks) in enumerate(slabs):
            outgoing[slot] = packed(hop, [shifted[k] for k in blocks])

    def exchange(number, half, parts=(1, 0)):
        if number:
            settle(halo_like(2), halo_send.at[half])
        for step in directions:
            part = 1 if step[2] else 0
            if part not in parts:
                continue
            push(
                ext.at[(number, half) + tuple(span_of(s, "source") for s in step)],
                ext.at[(number, half) + tuple(span_of(s, "target") for s in step)],
                halo_send.at[half],
                halo_recv.at[number % 2, half, part],
                step,
            )

    def halo_like(part):
        return matrix_t.at[0 : (80, 72, 152)[part] * 4 * WIDTH // 256]

    with jax.named_scope("w_barrier"):
        pl.semaphore_wait(barrier, len(greeted))
    for hop in hops:
        count = sum(1 for slab in slabs if slab[0] == hop)
        rows = slice(cargo_start[hop], cargo_start[hop] + count)
        push(outgoing.at[rows], incoming.at[rows], other_send.at[0], other_recv.at[0], hop)
    for half in range(HALVES):
        loads[half].wait()
        exchange(0, half)

    out_row = lax.broadcasted_iota(jnp.int32, (256, 256), 0)
    out_lane = lax.broadcasted_iota(jnp.int32, (256, 256), 1)
    same = ((out_row & 3) == (out_lane >> 6)) & ((out_row >> 2) == (out_lane & 63))
    pick = jnp.where(same, 1.0, 0.0).astype(bf16)

    with jax.named_scope("onsite"):
        spread = jnp.where(
            lax.broadcasted_iota(jnp.int32, (4, 256), 0) == (lane & 3), 1.0, 0.0
        )
        raw = onsite[...]
        raw = (0.5 * (raw + jnp.swapaxes(raw, 0, 1))).reshape(256, 4)
        wide = jnp.dot(
            raw, spread, precision=lax.Precision.HIGHEST, preferred_element_type=f32
        )
        keep = ((out_row >> 6) == (out_lane >> 6)) & (
            (out_row & 15) == ((out_lane >> 2) & 15)
        )
        wide = jnp.where(keep, wide, 0.0).reshape(4, 4, 16, 256)
        local = jnp.sum(jnp.sum(wide, axis=0), axis=1)
        wide = jnp.dot(
            levels[...].reshape(64, 4) - CENTRE,
            spread,
            precision=lax.Precision.HIGHEST,
            preferred_element_type=f32,
        )
        keep = out_row[0:64] == (out_lane[0:64] >> 2)
        level = jnp.sum(jnp.where(keep, wide, 0.0), axis=0, keepdims=True)
        level = jnp.sum(jnp.where(same, level, 0.0), axis=1, keepdims=True)
        diag[...] = jnp.broadcast_to(level, (256, WIDTH)).reshape(4, 4, 4, 4, WIDTH)

    near = [
        [(place[axis] >= e - 1) & (place[axis] <= e + 1) for e in WITH_RIM]
        for axis in range(3)
    ]

    def turned(chooser, span):
        across = (((1,), (1,)), ((), ()))
        return [
            lax.dot_general(chooser, part, across, preferred_element_type=f32).astype(bf16)
            for part in split(matrix_t[span, :])
        ]

    def build(chosen, first_row, rows, behind):
        table = {(0, 0, 0): local}
        for k, offset in enumerate(half_offsets):
            table[offset] = flipped[k]
            table[tuple(-o for o in offset)] = behind(k, offset)
        for axis in range(3):
            kind = jnp.where(place[axis] == 3, 0, place[axis])
            fresh = {}
            for key in table:
                picks = []
                for residue in range(3):
                    step = (key[axis] % 3 - residue + 1) % 3 - 1
                    picks.append(table[key[:axis] + (step,) + key[axis + 1 :]])
                fresh[key] = jnp.where(
                    kind == 0, picks[0], jnp.where(kind == 1, picks[1], picks[2])
                )
            table = fresh
        row = first_row
        for group in chosen:
            for ex in group[0]:
                for ey in group[1]:
                    both = near[0][ex + 1] & near[1][ey + 1]
                    for ez in group[2]:
                        key = tuple((e + 1) % 3 - 1 for e in (ex, ey, ez))
                        matrix_t[row : row + 4, :] = jnp.where(
                            both & near[2][ez + 1], table[key], 0.0
                        )
                        row += 4
        span = slice(first_row, first_row + rows)
        matrix_hi[:, span], matrix_lo[:, span] = turned(pick, span)

    def mirrored(k, offset):
        axes = [n for n in range(3) if offset[n]]

        def choose(position, hop):
            if position == len(axes):
                return unpacked(hop, k) if any(hop) else shifted[k]
            axis = axes[position]
            edge = 0 if offset[axis] > 0 else 3
            away = hop[:axis] + (offset[axis],) + hop[axis + 1 :]
            return jnp.where(
                place[axis] == edge, choose(position + 1, away), choose(position + 1, hop)
            )

        return choose(0, (0, 0, 0))

    def times(span, value):
        high, low = split(value)
        return (
            jnp.dot(matrix_hi[:, span], low, preferred_element_type=f32)
            + jnp.dot(matrix_lo[:, span], high, preferred_element_type=f32)
            + jnp.dot(matrix_hi[:, span], high, preferred_element_type=f32)
        )

    def core(number, half):
        return ext[number, half, 1:5, 1:5, 1:5]

    def before(number, half):
        partial[half] = times(slice(0, 256), core(number, half).reshape(256, WIDTH))

    def arrive(number, half, part):
        with jax.named_scope("w_halo%d_%d" % (2 * number + half, part)):
            settle(halo_like(part), halo_recv.at[number % 2, half, part])

    def advance(number, half, target, extra, line_between=False):
        arrive(number, half, 0)
        rim = jnp.concatenate(
            [
                ext[(number, half) + tuple(reach(v) for v in group)].reshape(-1, WIDTH)
                for group in groups[1:5]
            ],
            axis=0,
        )
        total = partial[half] + times(slice(256, 576), rim)
        total = total.reshape(4, 4, 4, 4, WIDTH) + diag[...] * core(number, half)
        target[...] = total if extra is None else total - extra
        if line_between:
            to_line(1)
        arrive(number, half, 1)
        for side in range(2):
            high, low = split(ext[number, half, :, :, 5 * side].reshape(144, WIDTH))
            part = jnp.dot(
                matrix_z[side],
                jnp.concatenate([low, high, high], axis=0),
                preferred_element_type=f32,
            )
            target[:, :, 3 * side] += part.reshape(4, 4, 4, WIDTH)

    def inner(number, half):
        return ext.at[number, half, 1:5, 1:5, 1:5]

    def product(left, right):
        return jnp.sum(jnp.sum(left * right, axis=(0, 1, 2)), axis=0, keepdims=True)

    stores = [None] * HALVES

    def keep_copy(source, target, number, half):
        if number:
            stores[half].wait()
        copy = pltpu.make_async_copy(
            source,
            target.at[:, :, :, :, half * WIDTH : half * WIDTH + WIDTH],
            store_sem.at[half],
        )
        copy.start()
        stores[half] = copy

    def lanes(half):
        return slice(half * WIDTH, half * WIDTH + WIDTH)

    own = (first_sum, sums)
    from_plane = (first_plane, plane_slots)
    along_line = (first_line, line_slots)

    def to_plane(group):
        settle(along_line[0] if group else outgoing, other_send.at[0])
        for index, step in enumerate(plane):
            push(
                own[group].at[0],
                from_plane[group].at[index],
                other_send.at[0],
                other_recv.at[1 + group],
                step,
            )

    def to_line(group):
        with jax.named_scope("w_plane%d" % group):
            settle(from_plane[group], other_recv.at[1 + group])
        own[group][1] = own[group][0] + jnp.sum(from_plane[group][...], axis=0)
        settle(from_plane[group], other_send.at[0])
        for index, step in enumerate(line):
            push(
                own[group].at[1],
                along_line[group].at[index],
                other_send.at[0],
                other_recv.at[3 + group],
                step,
            )

    def from_line(group):
        with jax.named_scope("w_line%d" % group):
            settle(along_line[group], other_recv.at[3 + group])
        return own[group][1] + jnp.sum(along_line[group][...], axis=0)

    for half in range(HALVES):
        keep_copy(ext.at[0, half, 1:5, 1:5, 1:5], zeroth_ref, 0, half)
    with jax.named_scope("inner"):
        build(groups[:2], 0, 352, lambda k, offset: shifted[k])
        for half in range(HALVES):
            before(0, half)
    for half in range(HALVES):
        first_sum[0, :, :, lanes(half)] = product(core(0, half), core(0, half))[None]
    to_plane(0)
    with jax.named_scope("w_coef"):
        settle(incoming, other_recv.at[0])
    with jax.named_scope("rim"):
        build(groups[2:], 352, 224, mirrored)
        for side in range(2):
            start = 576 + 144 * side
            layer_row = out_row[0:64]
            layer_lane = out_lane[0:64]
            chooser = (
                ((layer_row & 3) == (layer_lane >> 6))
                & ((layer_row >> 2) == ((layer_lane >> 2) & 15))
                & ((layer_lane & 3) == 3 * side)
            )
            high, low = turned(
                jnp.where(chooser, 1.0, 0.0).astype(bf16), slice(start, start + 144)
            )
            for index, part in enumerate((high, low, high)):
                matrix_z[side, :, 144 * index : 144 * index + 144] = part

    for half in range(HALVES):
        advance(0, half, inner(1, half), None)
        exchange(1, half)
        keep_copy(ext.at[1, half, 1:5, 1:5, 1:5], first_ref, 1, half)
        before(1, half)
        if half == 0:
            to_line(0)
        sums[0, 0, :, lanes(half)] = product(core(0, half), core(1, half))
        sums[0, 1, :, lanes(half)] = product(core(1, half), core(1, half))
    for half in range(HALVES):
        advance(1, half, inner(2, half), GAMMA1 * core(0, half))
        exchange(2, half)
        keep_copy(ext.at[2, half, 1:5, 1:5, 1:5], second_ref, 2, half)
        before(2, half)
        sums[0, 2, :, lanes(half)] = product(core(0, half), core(2, half))
        sums[0, 3, :, lanes(half)] = product(core(1, half), core(2, half))
        sums[0, 4, :, lanes(half)] = product(core(2, half), core(2, half))
    to_plane(1)
    g00 = from_line(0)[0]
    for half in range(HALVES):
        advance(2, half, last.at[half], GAMMA2 * core(1, half), half == HALVES - 1)
        final_sum[half] = product(core(2, half), last[half])
        settle(halo_like(2), halo_send.at[half])
        for index, step in enumerate(others):
            push(
                final_sum.at[half],
                final_slots.at[half, index],
                halo_send.at[half],
                final_recv.at[half],
                step,
            )
        keep_copy(last.at[half], third_ref, 3, half)
    rest = from_line(1)
    rr2, pq, weight, start, along = early_part(
        g00, rest[0], rest[2], rest[1], rest[3], rest[4], shift[...] + CENTRE
    )
    with jax.named_scope("w_stores"):
        for copy in stores:
            copy.wait()
        settle(along_line[1], other_send.at[0])
    totals = []
    for half in range(HALVES):
        with jax.named_scope("w_final%d" % half):
            settle(final_slots.at[half], final_recv.at[half])
        totals.append(final_sum[half] + jnp.sum(final_slots[half], axis=0))
    a2 = rr2 / (pq + weight * jnp.concatenate(totals, axis=1))
    for n in range(7):
        mix_ref[n : n + 1, :] = start[n] + a2 * along[n]
    for half in range(HALVES):
        settle(final_slots.at[half], halo_send.at[half])


def combine(zeroth_ref, first_ref, second_ref, third_ref, mix_ref, sol_ref, res_ref, sol, res, sem):
    copies = []
    for x in range(4):
        zeroth, first, second = zeroth_ref[x], first_ref[x], second_ref[x]
        sol[x] = mix_ref[0] * zeroth + mix_ref[1] * first + mix_ref[2] * second
        res[x] = (
            mix_ref[3] * zeroth
            + mix_ref[4] * first
            + mix_ref[5] * second
            + mix_ref[6] * third_ref[x]
        )
        copies.append(pltpu.make_async_copy(sol.at[x], sol_ref.at[x], sem.at[0, x]))
        copies.append(pltpu.make_async_copy(res.at[x], res_ref.at[x], sem.at[1, x]))
        for copy in copies[-2:]:
            copy.start()
    for copy in copies:
        copy.wait()


def solution(mesh):
    sizes = tuple(mesh.shape[name] for name in AXES)
    count = sizes[0] * sizes[1] * sizes[2]

    def per_device(right_side, bond_blocks, bond_open, onsite_blocks, orbital_levels, column_shift):
        vmem = pl.BlockSpec(memory_space=pltpu.VMEM)
        hbm = pl.BlockSpec(memory_space=pl.ANY)
        out = jax.ShapeDtypeStruct((4, 4, 4, 4, 256), f32)
        field = pltpu.VMEM((4, 4, 4, 4, 256), f32)
        kept = pl.pallas_call(
            functools.partial(kernel, sizes),
            out_shape=(field,) * 4 + (pltpu.VMEM((7, 256), f32),),
            in_specs=[hbm] * 6,
            out_specs=(hbm,) * 4 + (vmem,),
            scratch_shapes=[
                pltpu.VMEM((3, HALVES, 6, 6, 6, 4, WIDTH), f32),
                pltpu.VMEM((HALVES, 4, 4, 4, 4, WIDTH), f32),
                pltpu.VMEM((HALVES, 256, WIDTH), f32),
                pltpu.VMEM((4, 4, 4, 4, WIDTH), f32),
                pltpu.VMEM((4, 4, 4, 4, 4, 13), f32),
                pltpu.VMEM((4, 4, 4, 13), jnp.int32),
                pltpu.VMEM((4, 4, 4, 4, 4), f32),
                pltpu.VMEM((4, 4, 4, 4), f32),
                pltpu.VMEM((1, 256), f32),
                pltpu.VMEM((13, 4, 256), f32),
                pltpu.VMEM((13, 4, 256), f32),
                pltpu.VMEM((13, 4, 256), f32),
                pltpu.VMEM((CARGO, 4, 256), f32),
                pltpu.VMEM((CARGO, 4, 256), f32),
                pltpu.VMEM((864, 256), f32),
                pltpu.VMEM((256, 576), bf16),
                pltpu.VMEM((256, 576), bf16),
                pltpu.VMEM((2, 64, 432), bf16),
                pltpu.VMEM((2, 1, 1, 256), f32),
                pltpu.VMEM((sizes[0] * sizes[1] - 1, 1, 1, 256), f32),
                pltpu.VMEM((sizes[2] - 1, 1, 1, 256), f32),
                pltpu.VMEM((2, 5, 1, 256), f32),
                pltpu.VMEM((sizes[0] * sizes[1] - 1, 5, 1, 256), f32),
                pltpu.VMEM((sizes[2] - 1, 5, 1, 256), f32),
                pltpu.VMEM((HALVES, 1, WIDTH), f32),
                pltpu.VMEM((HALVES, count - 1, 1, WIDTH), f32),
                pltpu.SemaphoreType.DMA((5,)),
                pltpu.SemaphoreType.DMA((HALVES,)),
                pltpu.SemaphoreType.DMA((HALVES,)),
                pltpu.SemaphoreType.DMA((2, HALVES, 2)),
                pltpu.SemaphoreType.DMA((1,)),
                pltpu.SemaphoreType.DMA((5,)),
                pltpu.SemaphoreType.DMA((HALVES,)),
            ],
            compiler_params=pltpu.CompilerParams(collective_id=0, has_side_effects=True),
        )(
            right_side,
            jnp.transpose(bond_blocks, (1, 2, 3, 4, 5, 0)),
            jnp.transpose(bond_open, (1, 2, 3, 0)),
            onsite_blocks,
            orbital_levels,
            column_shift.reshape(1, 256),
        )
        return pl.pallas_call(
            combine,
            out_shape=(out, out),
            in_specs=[vmem] * 5,
            out_specs=(hbm, hbm),
            scratch_shapes=[
                pltpu.VMEM((4, 4, 4, 4, 256), f32),
                pltpu.VMEM((4, 4, 4, 4, 256), f32),
                pltpu.SemaphoreType.DMA((2, 4)),
            ],
        )(*[pltpu.with_memory_space_constraint(value, pltpu.VMEM) for value in kept])

    return jax.shard_map(
        per_device,
        mesh=mesh,
        in_specs=(
            P("gx", "gy", "gz", None, None),
            P(None, None, None, "gx", "gy", "gz"),
            P(None, "gx", "gy", "gz"),
            P(None, None, "gx", "gy", "gz"),
            P(None, "gx", "gy", "gz"),
            P(),
        ),
        out_specs=(P("gx", "gy", "gz", None, None), P("gx", "gy", "gz", None, None)),
        check_vma=False,
    )
```

```python
import functools

import jax
import jax.numpy as jnp
from jax import lax
from jax.experimental import pallas as pl
from jax.experimental.pallas import tpu as pltpu
from jax.sharding import PartitionSpec as P

f32 = jnp.float32
bf16 = jnp.bfloat16
MESH = pl.DeviceIdType.MESH

CENTRE = 1.95
GAMMA1 = 0.65 * 0.65 / 3.0
GAMMA2 = 0.65 * 0.65 * 4.0 / 15.0
HALVES = 2
WIDTH = 256 // HALVES
AXES = ("gx", "gy", "gz")

ALL = (-1, 0, 1)
every = [(i, j, k) for i in ALL for j in ALL for k in ALL]
half_offsets = [o for o in every if o > (0, 0, 0)]
directions = sorted(
    [o for o in every if o != (0, 0, 0)],
    key=lambda d: (-abs(d[2]), abs(d[0]) + abs(d[1])),
)
hops = sorted(
    {
        tuple(o[n] * keep[n] for n in range(3))
        for o in half_offsets
        for keep in [(i, j, k) for i in (0, 1) for j in (0, 1) for k in (0, 1)]
    }
    - {(0, 0, 0)},
    key=lambda d: (-abs(d[2]), d),
)
cargo = {
    hop: [
        k
        for k, o in enumerate(half_offsets)
        if all(hop[n] in (0, o[n]) for n in range(3))
    ]
    for hop in hops
}
cargo_slot, slabs = {}, []
cargo_start = {}
for hop in hops:
    cargo_start[hop] = len(slabs)
    for index, k in enumerate(cargo[hop]):
        if index % 4 == 0:
            slabs.append((hop, []))
        slabs[-1][1].append(k)
        cargo_slot[hop, k] = (len(slabs) - 1, index % 4)
CARGO = len(slabs)

INSIDE = range(0, 4)
WITH_RIM = range(-1, 5)
groups = [
    (INSIDE, INSIDE, INSIDE),
    ((4,), WITH_RIM, INSIDE),
    ((-1,), WITH_RIM, INSIDE),
    (INSIDE, (-1,), INSIDE),
    (INSIDE, (4,), INSIDE),
    (WITH_RIM, WITH_RIM, (-1,)),
    (WITH_RIM, WITH_RIM, (4,)),
]


def span_of(step, side):
    if step == 0:
        return slice(1, 5)
    if side == "source":
        return slice(4, 5) if step > 0 else slice(1, 2)
    return slice(0, 1) if step > 0 else slice(5, 6)


def reach(values):
    return slice(values[0] + 1, values[-1] + 2)


def split(value):
    high = value.astype(bf16)
    return high, (value - high.astype(f32)).astype(bf16)


def early_part(g00, g01, g02, g11, g12, g22, theta):
    g03 = g12 - GAMMA2 * g01
    g13 = g22 + GAMMA1 * g02 - GAMMA2 * g11
    a0 = g00 / (theta * g00 + g01)
    s0 = a0
    r0, r1 = 1.0 - a0 * theta, -a0
    rr1 = r0 * r0 * g00 + 2.0 * r0 * r1 * g01 + r1 * r1 * g11
    p0, p1 = r0 + rr1 / g00, r1
    q0, q1, q2 = theta * p0 + GAMMA1 * p1, p0 + theta * p1, p1
    pq = p0 * (q0 * g00 + q1 * g01 + q2 * g02) + p1 * (q0 * g01 + q1 * g11 + q2 * g12)
    a1 = rr1 / pq
    s0, s1 = s0 + a1 * p0, a1 * p1
    r0, r1, r2 = r0 - a1 * q0, r1 - a1 * q1, -a1 * q2
    rr2 = (
        r0 * (r0 * g00 + r1 * g01 + r2 * g02)
        + r1 * (r0 * g01 + r1 * g11 + r2 * g12)
        + r2 * (r0 * g02 + r1 * g12 + r2 * g22)
    )
    ratio = rr2 / rr1
    p0, p1, p2 = r0 + ratio * p0, r1 + ratio * p1, r2
    q0 = theta * p0 + GAMMA1 * p1
    q1 = p0 + theta * p1 + GAMMA2 * p2
    q2 = p1 + theta * p2
    q3 = p2
    pq = (
        p0 * (q0 * g00 + q1 * g01 + q2 * g02 + q3 * g03)
        + p1 * (q0 * g01 + q1 * g11 + q2 * g12 + q3 * g13)
        + p2 * (q0 * g02 + q1 * g12 + q2 * g22)
    )
    return rr2, pq, p2 * q3, (s0, s1, 0.0, r0, r1, r2, 0.0), (p0, p1, p2, -q0, -q1, -q2, -q3)


def kernel(
    sizes,
    right_ref,
    bond_ref,
    open_ref,
    onsite_ref,
    level_ref,
    shift_ref,
    zeroth_ref,
    first_ref,
    second_ref,
    third_ref,
    mix_ref,
    ext,
    last,
    partial,
    diag,
    bonds,
    opened,
    onsite,
    levels,
    shift,
    natural,
    flipped,
    shifted,
    outgoing,
    incoming,
    matrix_t,
    matrix_hi,
    matrix_lo,
    matrix_x,
    matrix_y,
    matrix_z,
    first_sum,
    first_plane,
    first_line,
    sums,
    plane_slots,
    line_slots,
    final_sum,
    final_slots,
    load_sem,
    store_sem,
    halo_send,
    halo_recv,
    other_send,
    other_recv,
    final_recv,
):
    me = [lax.axis_index(name) for name in AXES]
    side_refs = (matrix_x, matrix_y, matrix_z)

    def at(step):
        return tuple(lax.rem(me[n] + (step[n] + sizes[n]), sizes[n]) for n in range(3))

    def push(source, target, send, recv, step):
        pltpu.make_async_remote_copy(
            src_ref=source,
            dst_ref=target,
            send_sem=send,
            recv_sem=recv,
            device_id=at(step),
            device_id_type=MESH,
        ).start()

    def settle(like, sem):
        pltpu.make_async_copy(like, like, sem).wait()

    plane = [(i, j, 0) for i in range(sizes[0]) for j in range(sizes[1]) if (i, j) != (0, 0)]
    line = [(0, 0, k) for k in range(1, sizes[2])]
    others = [
        (i, j, k)
        for i in range(sizes[0])
        for j in range(sizes[1])
        for k in range(sizes[2])
        if (i, j, k) != (0, 0, 0)
    ]
    far = {0: 0, 1: 3, 2: 4, 3: 3, 4: 2}

    def path(step):
        return -(min(step[1], sizes[1] - step[1]) + far.get(min(step[2], sizes[2] - step[2]), 4))

    others.sort(key=path)
    greeted = {tuple(d[n] % sizes[n] for n in range(3)) for d in directions}
    greeted = sorted(greeted | set(plane) | set(line), key=lambda d: (path(d), d))


    loads = []
    for half in range(HALVES):
        loads.append(
            pltpu.make_async_copy(
                right_ref.at[:, :, :, :, half * WIDTH : half * WIDTH + WIDTH],
                ext.at[0, half, 1:5, 1:5, 1:5],
                store_sem.at[half],
            )
        )
    tables = [
        pltpu.make_async_copy(bond_ref, bonds, load_sem.at[0]),
        pltpu.make_async_copy(open_ref, opened, load_sem.at[1]),
        pltpu.make_async_copy(onsite_ref, onsite, load_sem.at[2]),
        pltpu.make_async_copy(level_ref, levels, load_sem.at[3]),
        pltpu.make_async_copy(shift_ref, shift, load_sem.at[4]),
    ]
    for copy in tables + loads:
        copy.start()
    barrier = pltpu.get_barrier_semaphore()
    with jax.named_scope("greet"):
        for step in greeted:
            pl.semaphore_signal(barrier, inc=1, device_id=at(step), device_id_type=MESH)

    lane = lax.broadcasted_iota(jnp.int32, (4, 256), 1)
    place = ((lane >> 4) & 3, (lane >> 2) & 3, lane & 3)

    def cyclic(value, axis, step):
        stride = (16, 4, 1)[axis]
        if step == 0:
            return value
        if step > 0:
            return jnp.where(
                place[axis] == 0,
                pltpu.roll(value, 256 - 3 * stride, 1),
                pltpu.roll(value, stride, 1),
            )
        return jnp.where(
            place[axis] == 3,
            pltpu.roll(value, 3 * stride, 1),
            pltpu.roll(value, 256 - stride, 1),
        )

    def layer(hop):
        axis = [n for n in range(3) if hop[n]][0]
        return axis, (16, 4, 1)[axis], 0 if hop[axis] > 0 else 3

    def packed(hop, values):
        axis, stride, edge = layer(hop)
        total = values[0]
        for index in range(1, len(values)):
            spot = (edge + index) % 4
            moved = pltpu.roll(values[index], (stride * (spot - edge)) % 256, 1)
            total = jnp.where(place[axis] == spot, moved, total)
        return total

    def unpacked(hop, k):
        axis, stride, edge = layer(hop)
        slot, index = cargo_slot[hop, k]
        spot = (edge + index) % 4
        value = incoming[slot]
        return value if index == 0 else pltpu.roll(value, (stride * (edge - spot)) % 256, 1)

    with jax.named_scope("tables"):
        for copy in tables:
            copy.wait()
        blocks = bonds[...] * opened[...].astype(f32)
        table = blocks.reshape(1024, 13).T
        for orb in range(4):
            natural[:, orb, :] = table[:, 256 * orb : 256 * orb + 256]
        table = jnp.swapaxes(blocks, 0, 1).reshape(1024, 13).T
        for orb in range(4):
            flipped[:, orb, :] = table[:, 256 * orb : 256 * orb + 256]
        for k, offset in enumerate(half_offsets):
            value = natural[k]
            for axis in range(3):
                value = cyclic(value, axis, offset[axis])
            shifted[k] = value
        for slot, (hop, blocks) in enumerate(slabs):
            outgoing[slot] = packed(hop, [shifted[k] for k in blocks])

    def exchange(number, half, parts=(1, 0)):
        if number:
            settle(halo_like(2), halo_send.at[half])
        for step in directions:
            part = 1 if step[2] else 0
            if part not in parts:
                continue
            push(
                ext.at[(number, half) + tuple(span_of(s, "source") for s in step)],
                ext.at[(number, half) + tuple(span_of(s, "target") for s in step)],
                halo_send.at[half],
                halo_recv.at[number % 2, half, part],
                step,
            )

    def halo_like(part):
        return matrix_t.at[0 : (80, 72, 152)[part] * 4 * WIDTH // 256]

    with jax.named_scope("w_barrier"):
        pl.semaphore_wait(barrier, len(greeted))
    for hop in hops:
        count = sum(1 for slab in slabs if slab[0] == hop)
        rows = slice(cargo_start[hop], cargo_start[hop] + count)
        push(outgoing.at[rows], incoming.at[rows], other_send.at[0], other_recv.at[0], hop)
    for half in range(HALVES):
        loads[half].wait()
        exchange(0, half)

    out_row = lax.broadcasted_iota(jnp.int32, (256, 256), 0)
    out_lane = lax.broadcasted_iota(jnp.int32, (256, 256), 1)
    same = ((out_row & 3) == (out_lane >> 6)) & ((out_row >> 2) == (out_lane & 63))
    pick = jnp.where(same, 1.0, 0.0).astype(bf16)

    with jax.named_scope("onsite"):
        spread = jnp.where(
            lax.broadcasted_iota(jnp.int32, (4, 256), 0) == (lane & 3), 1.0, 0.0
        )
        raw = onsite[...]
        raw = (0.5 * (raw + jnp.swapaxes(raw, 0, 1))).reshape(256, 4)
        wide = jnp.dot(
            raw, spread, precision=lax.Precision.HIGHEST, preferred_element_type=f32
        )
        keep = ((out_row >> 6) == (out_lane >> 6)) & (
            (out_row & 15) == ((out_lane >> 2) & 15)
        )
        wide = jnp.where(keep, wide, 0.0).reshape(4, 4, 16, 256)
        local = jnp.sum(jnp.sum(wide, axis=0), axis=1)
        wide = jnp.dot(
            levels[...].reshape(64, 4) - CENTRE,
            spread,
            precision=lax.Precision.HIGHEST,
            preferred_element_type=f32,
        )
        keep = out_row[0:64] == (out_lane[0:64] >> 2)
        level = jnp.sum(jnp.where(keep, wide, 0.0), axis=0, keepdims=True)
        level = jnp.sum(jnp.where(same, level, 0.0), axis=1, keepdims=True)
        diag[...] = jnp.broadcast_to(level, (256, WIDTH)).reshape(4, 4, 4, 4, WIDTH)

    near = [
        [(place[axis] >= e - 1) & (place[axis] <= e + 1) for e in WITH_RIM]
        for axis in range(3)
    ]

    def turned(chooser, span):
        across = (((1,), (1,)), ((), ()))
        return [
            lax.dot_general(chooser, part, across, preferred_element_type=f32).astype(bf16)
            for part in split(matrix_t[span, :])
        ]

    def build(chosen, first_row, behind):
        table = {(0, 0, 0): local}
        for k, offset in enumerate(half_offsets):
            table[offset] = flipped[k]
            table[tuple(-o for o in offset)] = behind(k, offset)
        for axis in range(3):
            kind = jnp.where(place[axis] == 3, 0, place[axis])
            fresh = {}
            for key in table:
                picks = []
                for residue in range(3):
                    step = (key[axis] % 3 - residue + 1) % 3 - 1
                    picks.append(table[key[:axis] + (step,) + key[axis + 1 :]])
                fresh[key] = jnp.where(
                    kind == 0, picks[0], jnp.where(kind == 1, picks[1], picks[2])
                )
            table = fresh
        row = first_row
        for group in chosen:
            for ex in group[0]:
                for ey in group[1]:
                    both = near[0][ex + 1] & near[1][ey + 1]
                    for ez in group[2]:
                        key = tuple((e + 1) % 3 - 1 for e in (ex, ey, ez))
                        matrix_t[row : row + 4, :] = jnp.where(
                            both & near[2][ez + 1], table[key], 0.0
                        )
                        row += 4

    layers = (((3, 5), (0, 0)), ((0, 0), (3, 5)), ((0, 0), (3, 5)))
    starts = ((256, 352, 448), (448, 512, 576), (576, 720, 864))

    def side_matrix(axis, side):
        row, at_lane = out_row[0:64], out_lane[0:64]
        x, y, z = (at_lane >> 4) & 3, (at_lane >> 2) & 3, at_lane & 3
        along = ((y, z), (x, z), (x, y))[axis]
        chooser = (
            ((row & 3) == (at_lane >> 6))
            & ((row >> 4) == along[0])
            & (((row >> 2) & 3) == along[1])
            & ((x, y, z)[axis] == layers[axis][side][0])
        )
        first, end = starts[axis][side : side + 2]
        high, low = turned(jnp.where(chooser, 1.0, 0.0).astype(bf16), slice(first, end))
        for index, part in enumerate((high, low, high)):
            span = slice((end - first) * index, (end - first) * (index + 1))
            side_refs[axis][side, :, span] = part

    def mirrored(k, offset):
        axes = [n for n in range(3) if offset[n]]

        def choose(position, hop):
            if position == len(axes):
                return unpacked(hop, k) if any(hop) else shifted[k]
            axis = axes[position]
            edge = 0 if offset[axis] > 0 else 3
            away = hop[:axis] + (offset[axis],) + hop[axis + 1 :]
            return jnp.where(
                place[axis] == edge, choose(position + 1, away), choose(position + 1, hop)
            )

        return choose(0, (0, 0, 0))

    def times(span, value):
        high, low = split(value)
        return (
            jnp.dot(matrix_hi[:, span], low, preferred_element_type=f32)
            + jnp.dot(matrix_lo[:, span], high, preferred_element_type=f32)
            + jnp.dot(matrix_hi[:, span], high, preferred_element_type=f32)
        )

    def core(number, half):
        return ext[number, half, 1:5, 1:5, 1:5]

    def before(number, half):
        total = times(slice(0, 256), core(number, half).reshape(256, WIDTH))
        total = total.reshape(4, 4, 4, 4, WIDTH) + diag[...] * core(number, half)
        if number:
            total = total - (GAMMA1, GAMMA2)[number - 1] * core(number - 1, half)
        partial[half] = total

    def arrive(number, half, part):
        with jax.named_scope("w_halo%d_%d" % (2 * number + half, part)):
            settle(halo_like(part), halo_recv.at[number % 2, half, part])

    def advance(number, half, target):
        def add(axis):
            for side in range(2):
                out, rim = layers[axis][side]
                where = [slice(None)] * 3
                where[axis] = out
                if axis == 0:
                    value = ext[number, half, rim, :, 1:5]
                elif axis == 1:
                    value = ext[number, half, 1:5, rim, 1:5]
                else:
                    value = ext[number, half, :, :, rim]
                high, low = split(value.reshape(-1, WIDTH))
                part = jnp.dot(
                    side_refs[axis][side],
                    jnp.concatenate([low, high, high], axis=0),
                    preferred_element_type=f32,
                )
                target[tuple(where)] += part.reshape(4, 4, 4, WIDTH)

        target[...] = partial[half]
        arrive(number, half, 0)
        add(0)
        add(1)
        arrive(number, half, 1)
        add(2)

    def inner(number, half):
        return ext.at[number, half, 1:5, 1:5, 1:5]

    def product(left, right):
        return jnp.sum(jnp.sum(left * right, axis=(0, 1, 2)), axis=0, keepdims=True)

    stores = [None] * HALVES

    def keep_copy(source, target, number, half):
        if number:
            stores[half].wait()
        copy = pltpu.make_async_copy(
            source,
            target.at[:, :, :, :, half * WIDTH : half * WIDTH + WIDTH],
            store_sem.at[half],
        )
        copy.start()
        stores[half] = copy

    def lanes(half):
        return slice(half * WIDTH, half * WIDTH + WIDTH)

    own = (first_sum, sums)
    from_plane = (first_plane, plane_slots)
    along_line = (first_line, line_slots)

    def to_plane(group):
        settle(along_line[0] if group else outgoing, other_send.at[0])
        for index, step in enumerate(plane):
            push(
                own[group].at[0],
                from_plane[group].at[index],
                other_send.at[0],
                other_recv.at[1 + group],
                step,
            )

    def to_line(group):
        with jax.named_scope("w_plane%d" % group):
            settle(from_plane[group], other_recv.at[1 + group])
        own[group][1] = own[group][0] + jnp.sum(from_plane[group][...], axis=0)
        settle(from_plane[group], other_send.at[0])
        for index, step in enumerate(line):
            push(
                own[group].at[1],
                along_line[group].at[index],
                other_send.at[0],
                other_recv.at[3 + group],
                step,
            )

    def from_line(group):
        with jax.named_scope("w_line%d" % group):
            settle(along_line[group], other_recv.at[3 + group])
        return own[group][1] + jnp.sum(along_line[group][...], axis=0)

    for half in range(HALVES):
        keep_copy(ext.at[0, half, 1:5, 1:5, 1:5], zeroth_ref, 0, half)
    with jax.named_scope("inner"):
        build(groups[:2], 0, lambda k, offset: shifted[k])
        matrix_hi[...], matrix_lo[...] = turned(pick, slice(0, 256))
        side_matrix(0, 0)
        for half in range(HALVES):
            before(0, half)
    for half in range(HALVES):
        first_sum[0, :, :, lanes(half)] = product(core(0, half), core(0, half))[None]
    to_plane(0)
    with jax.named_scope("w_coef"):
        settle(incoming, other_recv.at[0])
    with jax.named_scope("rim"):
        build(groups[2:], 352, mirrored)
        for axis, side in ((0, 1), (1, 0), (1, 1), (2, 0), (2, 1)):
            side_matrix(axis, side)

    for half in range(HALVES):
        advance(0, half, inner(1, half))
        exchange(1, half)
        keep_copy(ext.at[1, half, 1:5, 1:5, 1:5], first_ref, 1, half)
        before(1, half)
        if half == 0:
            to_line(0)
        sums[0, 0, :, lanes(half)] = product(core(0, half), core(1, half))
        sums[0, 1, :, lanes(half)] = product(core(1, half), core(1, half))
    for half in range(HALVES):
        advance(1, half, inner(2, half))
        exchange(2, half)
        keep_copy(ext.at[2, half, 1:5, 1:5, 1:5], second_ref, 2, half)
        before(2, half)
        sums[0, 2, :, lanes(half)] = product(core(0, half), core(2, half))
        sums[0, 3, :, lanes(half)] = product(core(1, half), core(2, half))
        sums[0, 4, :, lanes(half)] = product(core(2, half), core(2, half))
    to_plane(1)
    g00 = from_line(0)[0]
    for half in range(HALVES):
        advance(2, half, last.at[half])
        final_sum[half] = product(core(2, half), last[half])
        settle(halo_like(2), halo_send.at[half])
        for index, step in enumerate(others):
            if half == HALVES - 1 and index == 60:
                to_line(1)
            push(
                final_sum.at[half],
                final_slots.at[half, index],
                halo_send.at[half],
                final_recv.at[half],
                step,
            )
        keep_copy(last.at[half], third_ref, 3, half)
    rest = from_line(1)
    rr2, pq, weight, start, along = early_part(
        g00, rest[0], rest[2], rest[1], rest[3], rest[4], shift[...] + CENTRE
    )
    with jax.named_scope("w_stores"):
        for copy in stores:
            copy.wait()
        settle(along_line[1], other_send.at[0])
    totals = []
    for half in range(HALVES):
        with jax.named_scope("w_final%d" % half):
            settle(final_slots.at[half], final_recv.at[half])
        totals.append(final_sum[half] + jnp.sum(final_slots[half], axis=0))
    a2 = rr2 / (pq + weight * jnp.concatenate(totals, axis=1))
    for n in range(7):
        mix_ref[n : n + 1, :] = start[n] + a2 * along[n]
    for half in range(HALVES):
        settle(final_slots.at[half], halo_send.at[half])


def combine(zeroth_ref, first_ref, second_ref, third_ref, mix_ref, sol_ref, res_ref, sol, res, sem):
    for part in [(slice(x, x + 1), slice(y, y + 2)) for x in range(4) for y in (0, 2)]:
        zeroth, first, second = zeroth_ref[part], first_ref[part], second_ref[part]
        res[part] = (
            mix_ref[3] * zeroth
            + mix_ref[4] * first
            + mix_ref[5] * second
            + mix_ref[6] * third_ref[part]
        )
        pltpu.make_async_copy(res.at[part], res_ref.at[part], sem.at[1]).start()
        sol[part] = mix_ref[0] * zeroth + mix_ref[1] * first + mix_ref[2] * second
        pltpu.make_async_copy(sol.at[part], sol_ref.at[part], sem.at[0]).start()
    pltpu.make_async_copy(sol, sol_ref, sem.at[0]).wait()
    pltpu.make_async_copy(res, res_ref, sem.at[1]).wait()


def solution(mesh):
    sizes = tuple(mesh.shape[name] for name in AXES)
    count = sizes[0] * sizes[1] * sizes[2]

    def per_device(right_side, bond_blocks, bond_open, onsite_blocks, orbital_levels, column_shift):
        vmem = pl.BlockSpec(memory_space=pltpu.VMEM)
        hbm = pl.BlockSpec(memory_space=pl.ANY)
        out = jax.ShapeDtypeStruct((4, 4, 4, 4, 256), f32)
        field = pltpu.VMEM((4, 4, 4, 4, 256), f32)
        kept = pl.pallas_call(
            functools.partial(kernel, sizes),
            out_shape=(field,) * 4 + (pltpu.VMEM((7, 256), f32),),
            in_specs=[hbm] * 6,
            out_specs=(hbm,) * 4 + (vmem,),
            scratch_shapes=[
                pltpu.VMEM((3, HALVES, 6, 6, 6, 4, WIDTH), f32),
                pltpu.VMEM((HALVES, 4, 4, 4, 4, WIDTH), f32),
                pltpu.VMEM((HALVES, 4, 4, 4, 4, WIDTH), f32),
                pltpu.VMEM((4, 4, 4, 4, WIDTH), f32),
                pltpu.VMEM((4, 4, 4, 4, 4, 13), f32),
                pltpu.VMEM((4, 4, 4, 13), jnp.int32),
                pltpu.VMEM((4, 4, 4, 4, 4), f32),
                pltpu.VMEM((4, 4, 4, 4), f32),
                pltpu.VMEM((1, 256), f32),
                pltpu.VMEM((13, 4, 256), f32),
                pltpu.VMEM((13, 4, 256), f32),
                pltpu.VMEM((13, 4, 256), f32),
                pltpu.VMEM((CARGO, 4, 256), f32),
                pltpu.VMEM((CARGO, 4, 256), f32),
                pltpu.VMEM((864, 256), f32),
                pltpu.VMEM((256, 256), bf16),
                pltpu.VMEM((256, 256), bf16),
                pltpu.VMEM((2, 64, 288), bf16),
                pltpu.VMEM((2, 64, 192), bf16),
                pltpu.VMEM((2, 64, 432), bf16),
                pltpu.VMEM((2, 1, 1, 256), f32),
                pltpu.VMEM((sizes[0] * sizes[1] - 1, 1, 1, 256), f32),
                pltpu.VMEM((sizes[2] - 1, 1, 1, 256), f32),
                pltpu.VMEM((2, 5, 1, 256), f32),
                pltpu.VMEM((sizes[0] * sizes[1] - 1, 5, 1, 256), f32),
                pltpu.VMEM((sizes[2] - 1, 5, 1, 256), f32),
                pltpu.VMEM((HALVES, 1, WIDTH), f32),
                pltpu.VMEM((HALVES, count - 1, 1, WIDTH), f32),
                pltpu.SemaphoreType.DMA((5,)),
                pltpu.SemaphoreType.DMA((HALVES,)),
                pltpu.SemaphoreType.DMA((HALVES,)),
                pltpu.SemaphoreType.DMA((2, HALVES, 2)),
                pltpu.SemaphoreType.DMA((1,)),
                pltpu.SemaphoreType.DMA((5,)),
                pltpu.SemaphoreType.DMA((HALVES,)),
            ],
            compiler_params=pltpu.CompilerParams(collective_id=0, has_side_effects=True),
        )(
            right_side,
            jnp.transpose(bond_blocks, (1, 2, 3, 4, 5, 0)),
            jnp.transpose(bond_open, (1, 2, 3, 0)),
            onsite_blocks,
            orbital_levels,
            column_shift.reshape(1, 256),
        )
        return pl.pallas_call(
            combine,
            out_shape=(out, out),
            in_specs=[vmem] * 5,
            out_specs=(hbm, hbm),
            scratch_shapes=[
                pltpu.VMEM((4, 4, 4, 4, 256), f32),
                pltpu.VMEM((4, 4, 4, 4, 256), f32),
                pltpu.SemaphoreType.DMA((2,)),
            ],
        )(*[pltpu.with_memory_space_constraint(value, pltpu.VMEM) for value in kept])

    return jax.shard_map(
        per_device,
        mesh=mesh,
        in_specs=(
            P("gx", "gy", "gz", None, None),
            P(None, None, None, "gx", "gy", "gz"),
            P(None, "gx", "gy", "gz"),
            P(None, None, "gx", "gy", "gz"),
            P(None, "gx", "gy", "gz"),
            P(),
        ),
        out_specs=(P("gx", "gy", "gz", None, None), P("gx", "gy", "gz", None, None)),
        check_vma=False,
    )
```

```python
import functools

import jax
import jax.numpy as jnp
from jax import lax
from jax.experimental import pallas as pl
from jax.experimental.pallas import tpu as pltpu
from jax.sharding import PartitionSpec as P

f32 = jnp.float32
bf16 = jnp.bfloat16
MESH = pl.DeviceIdType.MESH

CENTRE = 1.95
GAMMA1 = 0.65 * 0.65 / 3.0
GAMMA2 = 0.65 * 0.65 * 4.0 / 15.0
HALVES = 2
WIDTH = 256 // HALVES
AXES = ("gx", "gy", "gz")

ALL = (-1, 0, 1)
every = [(i, j, k) for i in ALL for j in ALL for k in ALL]
half_offsets = [o for o in every if o > (0, 0, 0)]
directions = sorted(
    [o for o in every if o != (0, 0, 0)],
    key=lambda d: (-abs(d[2]), abs(d[0]) + abs(d[1])),
)
hops = sorted(
    {
        tuple(o[n] * keep[n] for n in range(3))
        for o in half_offsets
        for keep in [(i, j, k) for i in (0, 1) for j in (0, 1) for k in (0, 1)]
    }
    - {(0, 0, 0)},
    key=lambda d: (-abs(d[2]), d),
)
cargo = {
    hop: [
        k
        for k, o in enumerate(half_offsets)
        if all(hop[n] in (0, o[n]) for n in range(3))
    ]
    for hop in hops
}
cargo_slot, slabs = {}, []
cargo_start = {}
for hop in hops:
    cargo_start[hop] = len(slabs)
    for index, k in enumerate(cargo[hop]):
        if index % 4 == 0:
            slabs.append((hop, []))
        slabs[-1][1].append(k)
        cargo_slot[hop, k] = (len(slabs) - 1, index % 4)
CARGO = len(slabs)

INSIDE = range(0, 4)
WITH_RIM = range(-1, 5)
groups = [
    (INSIDE, INSIDE, INSIDE),
    ((4,), WITH_RIM, INSIDE),
    ((-1,), WITH_RIM, INSIDE),
    (INSIDE, (-1,), INSIDE),
    (INSIDE, (4,), INSIDE),
    (WITH_RIM, WITH_RIM, (-1,)),
    (WITH_RIM, WITH_RIM, (4,)),
]


def span_of(step, side):
    if step == 0:
        return slice(1, 5)
    if side == "source":
        return slice(4, 5) if step > 0 else slice(1, 2)
    return slice(0, 1) if step > 0 else slice(5, 6)


def reach(values):
    return slice(values[0] + 1, values[-1] + 2)


def split(value):
    high = value.astype(bf16)
    return high, (value - high.astype(f32)).astype(bf16)


def early_part(g00, g01, g02, g11, g12, g22, theta):
    g03 = g12 - GAMMA2 * g01
    g13 = g22 + GAMMA1 * g02 - GAMMA2 * g11
    a0 = g00 / (theta * g00 + g01)
    s0 = a0
    r0, r1 = 1.0 - a0 * theta, -a0
    rr1 = r0 * r0 * g00 + 2.0 * r0 * r1 * g01 + r1 * r1 * g11
    p0, p1 = r0 + rr1 / g00, r1
    q0, q1, q2 = theta * p0 + GAMMA1 * p1, p0 + theta * p1, p1
    pq = p0 * (q0 * g00 + q1 * g01 + q2 * g02) + p1 * (q0 * g01 + q1 * g11 + q2 * g12)
    a1 = rr1 / pq
    s0, s1 = s0 + a1 * p0, a1 * p1
    r0, r1, r2 = r0 - a1 * q0, r1 - a1 * q1, -a1 * q2
    rr2 = (
        r0 * (r0 * g00 + r1 * g01 + r2 * g02)
        + r1 * (r0 * g01 + r1 * g11 + r2 * g12)
        + r2 * (r0 * g02 + r1 * g12 + r2 * g22)
    )
    ratio = rr2 / rr1
    p0, p1, p2 = r0 + ratio * p0, r1 + ratio * p1, r2
    q0 = theta * p0 + GAMMA1 * p1
    q1 = p0 + theta * p1 + GAMMA2 * p2
    q2 = p1 + theta * p2
    q3 = p2
    pq = (
        p0 * (q0 * g00 + q1 * g01 + q2 * g02 + q3 * g03)
        + p1 * (q0 * g01 + q1 * g11 + q2 * g12 + q3 * g13)
        + p2 * (q0 * g02 + q1 * g12 + q2 * g22)
    )
    return rr2, pq, p2 * q3, (s0, s1, 0.0, r0, r1, r2, 0.0), (p0, p1, p2, -q0, -q1, -q2, -q3)


def kernel(
    sizes,
    right_ref,
    bond_ref,
    open_ref,
    onsite_ref,
    level_ref,
    shift_ref,
    zeroth_ref,
    first_ref,
    second_ref,
    third_ref,
    mix_ref,
    ext,
    last,
    partial,
    diag,
    bonds,
    opened,
    onsite,
    levels,
    shift,
    natural,
    flipped,
    shifted,
    outgoing,
    incoming,
    matrix_t,
    matrix_hi,
    matrix_lo,
    matrix_x,
    matrix_y,
    matrix_z,
    first_sum,
    first_plane,
    first_line,
    sums,
    plane_slots,
    line_slots,
    final_sum,
    final_slots,
    load_sem,
    store_sem,
    halo_send,
    halo_recv,
    other_send,
    other_recv,
    final_recv,
):
    me = [lax.axis_index(name) for name in AXES]
    side_refs = (matrix_x, matrix_y, matrix_z)

    def at(step):
        return tuple(lax.rem(me[n] + (step[n] + sizes[n]), sizes[n]) for n in range(3))

    def push(source, target, send, recv, step):
        pltpu.make_async_remote_copy(
            src_ref=source,
            dst_ref=target,
            send_sem=send,
            recv_sem=recv,
            device_id=at(step),
            device_id_type=MESH,
        ).start()

    def settle(like, sem):
        pltpu.make_async_copy(like, like, sem).wait()

    plane = [(i, j, 0) for i in range(sizes[0]) for j in range(sizes[1]) if (i, j) != (0, 0)]
    line = [(0, 0, k) for k in range(1, sizes[2])]
    others = [
        (i, j, k)
        for i in range(sizes[0])
        for j in range(sizes[1])
        for k in range(sizes[2])
        if (i, j, k) != (0, 0, 0)
    ]
    far = {0: 0, 1: 3, 2: 4, 3: 3, 4: 2}

    def path(step):
        return -(min(step[1], sizes[1] - step[1]) + far.get(min(step[2], sizes[2] - step[2]), 4))

    others.sort(key=path)
    greeted = {tuple(d[n] % sizes[n] for n in range(3)) for d in directions}
    greeted = sorted(greeted | set(plane) | set(line), key=lambda d: (path(d), d))


    loads = []
    for half in range(HALVES):
        loads.append(
            pltpu.make_async_copy(
                right_ref.at[:, :, :, :, half * WIDTH : half * WIDTH + WIDTH],
                ext.at[0, half, 1:5, 1:5, 1:5],
                store_sem.at[half],
            )
        )
    tables = [
        pltpu.make_async_copy(bond_ref, bonds, load_sem.at[0]),
        pltpu.make_async_copy(open_ref, opened, load_sem.at[1]),
        pltpu.make_async_copy(onsite_ref, onsite, load_sem.at[2]),
        pltpu.make_async_copy(level_ref, levels, load_sem.at[3]),
        pltpu.make_async_copy(shift_ref, shift, load_sem.at[4]),
    ]
    for copy in tables + loads:
        copy.start()
    barrier = pltpu.get_barrier_semaphore()
    with jax.named_scope("greet"):
        for step in greeted:
            pl.semaphore_signal(barrier, inc=1, device_id=at(step), device_id_type=MESH)

    lane = lax.broadcasted_iota(jnp.int32, (4, 256), 1)
    place = ((lane >> 4) & 3, (lane >> 2) & 3, lane & 3)

    def cyclic(value, axis, step):
        stride = (16, 4, 1)[axis]
        if step == 0:
            return value
        if step > 0:
            return jnp.where(
                place[axis] == 0,
                pltpu.roll(value, 256 - 3 * stride, 1),
                pltpu.roll(value, stride, 1),
            )
        return jnp.where(
            place[axis] == 3,
            pltpu.roll(value, 3 * stride, 1),
            pltpu.roll(value, 256 - stride, 1),
        )

    def layer(hop):
        axis = [n for n in range(3) if hop[n]][0]
        return axis, (16, 4, 1)[axis], 0 if hop[axis] > 0 else 3

    def packed(hop, values):
        axis, stride, edge = layer(hop)
        total = values[0]
        for index in range(1, len(values)):
            spot = (edge + index) % 4
            moved = pltpu.roll(values[index], (stride * (spot - edge)) % 256, 1)
            total = jnp.where(place[axis] == spot, moved, total)
        return total

    def unpacked(hop, k):
        axis, stride, edge = layer(hop)
        slot, index = cargo_slot[hop, k]
        spot = (edge + index) % 4
        value = incoming[slot]
        return value if index == 0 else pltpu.roll(value, (stride * (edge - spot)) % 256, 1)

    with jax.named_scope("tables"):
        for copy in tables:
            copy.wait()
        blocks = bonds[...] * opened[...].astype(f32)
        table = blocks.reshape(1024, 13).T
        for orb in range(4):
            natural[0:13, orb, :] = table[:, 256 * orb : 256 * orb + 256]
        table = jnp.swapaxes(blocks, 0, 1).reshape(1024, 13).T
        for orb in range(4):
            flipped[0:13, orb, :] = table[:, 256 * orb : 256 * orb + 256]
        for k, offset in enumerate(half_offsets):
            value = natural[k]
            for axis in range(3):
                value = cyclic(value, axis, offset[axis])
            shifted[k] = value
        for slot, (hop, blocks) in enumerate(slabs):
            outgoing[slot] = packed(hop, [shifted[k] for k in blocks])

    def exchange(number, half, parts=(1, 0)):
        if number:
            settle(halo_like(2), halo_send.at[half])
        for step in directions:
            part = 1 if step[2] else 0
            if part not in parts:
                continue
            push(
                ext.at[(number, half) + tuple(span_of(s, "source") for s in step)],
                ext.at[(number, half) + tuple(span_of(s, "target") for s in step)],
                halo_send.at[half],
                halo_recv.at[number % 2, half, part],
                step,
            )

    def halo_like(part):
        return matrix_t.at[0 : (80, 72, 152)[part] * 4 * WIDTH // 256]

    with jax.named_scope("w_barrier"):
        pl.semaphore_wait(barrier, len(greeted))
    for hop in hops:
        count = sum(1 for slab in slabs if slab[0] == hop)
        rows = slice(cargo_start[hop], cargo_start[hop] + count)
        push(outgoing.at[rows], incoming.at[rows], other_send.at[0], other_recv.at[0], hop)
    for half in range(HALVES):
        loads[half].wait()
        exchange(0, half)

    out_row = lax.broadcasted_iota(jnp.int32, (256, 256), 0)
    out_lane = lax.broadcasted_iota(jnp.int32, (256, 256), 1)
    same = ((out_row & 3) == (out_lane >> 6)) & ((out_row >> 2) == (out_lane & 63))
    pick = jnp.where(same, 1.0, 0.0).astype(bf16)

    with jax.named_scope("onsite"):
        spread = jnp.where(
            lax.broadcasted_iota(jnp.int32, (4, 256), 0) == (lane & 3), 1.0, 0.0
        )
        raw = onsite[...]
        raw = (0.5 * (raw + jnp.swapaxes(raw, 0, 1))).reshape(256, 4)
        wide = jnp.dot(
            raw, spread, precision=lax.Precision.HIGHEST, preferred_element_type=f32
        )
        keep = ((out_row >> 6) == (out_lane >> 6)) & (
            (out_row & 15) == ((out_lane >> 2) & 15)
        )
        wide = jnp.where(keep, wide, 0.0).reshape(4, 4, 16, 256)
        local = jnp.sum(jnp.sum(wide, axis=0), axis=1)
        wide = jnp.dot(
            levels[...].reshape(64, 4) - CENTRE,
            spread,
            precision=lax.Precision.HIGHEST,
            preferred_element_type=f32,
        )
        keep = out_row[0:64] == (out_lane[0:64] >> 2)
        level = jnp.sum(jnp.where(keep, wide, 0.0), axis=0, keepdims=True)
        level = jnp.sum(jnp.where(same, level, 0.0), axis=1, keepdims=True)
        diag[...] = jnp.broadcast_to(level, (256, WIDTH)).reshape(4, 4, 4, 4, WIDTH)

    near = [
        [(place[axis] >= e - 1) & (place[axis] <= e + 1) for e in WITH_RIM]
        for axis in range(3)
    ]

    def turned(chooser, span):
        across = (((1,), (1,)), ((), ()))
        return [
            lax.dot_general(chooser, part, across, preferred_element_type=f32).astype(bf16)
            for part in split(matrix_t[span, :])
        ]

    def build(chosen, first_row, behind):
        table = {(0, 0, 0): local}
        for k, offset in enumerate(half_offsets):
            table[offset] = flipped[k]
            table[tuple(-o for o in offset)] = behind(k, offset)
        for axis in range(3):
            kind = jnp.where(place[axis] == 3, 0, place[axis])
            fresh = {}
            for key in table:
                picks = []
                for residue in range(3):
                    step = (key[axis] % 3 - residue + 1) % 3 - 1
                    picks.append(table[key[:axis] + (step,) + key[axis + 1 :]])
                fresh[key] = jnp.where(
                    kind == 0, picks[0], jnp.where(kind == 1, picks[1], picks[2])
                )
            table = fresh
        row = first_row
        for group in chosen:
            for ex in group[0]:
                for ey in group[1]:
                    both = near[0][ex + 1] & near[1][ey + 1]
                    for ez in group[2]:
                        key = tuple((e + 1) % 3 - 1 for e in (ex, ey, ez))
                        matrix_t[row : row + 4, :] = jnp.where(
                            both & near[2][ez + 1], table[key], 0.0
                        )
                        row += 4

    layers = (((3, 5), (0, 0)), ((0, 0), (3, 5)), ((0, 0), (3, 5)))
    starts = ((256, 352, 448), (448, 512, 576), (576, 720, 864))

    def side_matrix(axis, side):
        row, at_lane = out_row[0:64], out_lane[0:64]
        x, y, z = (at_lane >> 4) & 3, (at_lane >> 2) & 3, at_lane & 3
        along = ((y, z), (x, z), (x, y))[axis]
        chooser = (
            ((row & 3) == (at_lane >> 6))
            & ((row >> 4) == along[0])
            & (((row >> 2) & 3) == along[1])
            & ((x, y, z)[axis] == layers[axis][side][0])
        )
        first, end = starts[axis][side : side + 2]
        high, low = turned(jnp.where(chooser, 1.0, 0.0).astype(bf16), slice(first, end))
        for index, part in enumerate((high, low, high)):
            span = slice((end - first) * index, (end - first) * (index + 1))
            side_refs[axis][side, :, span] = part

    def mirrored(k, offset):
        axes = [n for n in range(3) if offset[n]]

        def choose(position, hop):
            if position == len(axes):
                return unpacked(hop, k) if any(hop) else shifted[k]
            axis = axes[position]
            edge = 0 if offset[axis] > 0 else 3
            away = hop[:axis] + (offset[axis],) + hop[axis + 1 :]
            return jnp.where(
                place[axis] == edge, choose(position + 1, away), choose(position + 1, hop)
            )

        return choose(0, (0, 0, 0))

    def times(span, value):
        high, low = split(value)
        return (
            jnp.dot(matrix_hi[:, span], low, preferred_element_type=f32)
            + jnp.dot(matrix_lo[:, span], high, preferred_element_type=f32)
            + jnp.dot(matrix_hi[:, span], high, preferred_element_type=f32)
        )

    def core(number, half):
        return ext[number, half, 1:5, 1:5, 1:5]

    def before(number, half):
        total = times(slice(0, 256), core(number, half).reshape(256, WIDTH))
        total = total.reshape(4, 4, 4, 4, WIDTH) + diag[...] * core(number, half)
        if number:
            total = total - (GAMMA1, GAMMA2)[number - 1] * core(number - 1, half)
        partial[half] = total

    def arrive(number, half, part):
        with jax.named_scope("w_halo%d_%d" % (2 * number + half, part)):
            settle(halo_like(part), halo_recv.at[number % 2, half, part])

    def advance(number, half, target):
        def add(axis):
            for side in range(2):
                out, rim = layers[axis][side]
                where = [slice(None)] * 3
                where[axis] = out
                if axis == 0:
                    value = ext[number, half, rim, :, 1:5]
                elif axis == 1:
                    value = ext[number, half, 1:5, rim, 1:5]
                else:
                    value = ext[number, half, :, :, rim]
                high, low = split(value.reshape(-1, WIDTH))
                part = jnp.dot(
                    side_refs[axis][side],
                    jnp.concatenate([low, high, high], axis=0),
                    preferred_element_type=f32,
                )
                target[tuple(where)] += part.reshape(4, 4, 4, WIDTH)

        target[...] = partial[half]
        arrive(number, half, 0)
        add(0)
        add(1)
        arrive(number, half, 1)
        add(2)

    def inner(number, half):
        return ext.at[number, half, 1:5, 1:5, 1:5]

    def product(left, right):
        return jnp.sum(jnp.sum(left * right, axis=(0, 1, 2)), axis=0, keepdims=True)

    stores = [None] * HALVES

    def keep_copy(source, target, number, half):
        if number:
            stores[half].wait()
        copy = pltpu.make_async_copy(
            source,
            target.at[:, :, :, :, half * WIDTH : half * WIDTH + WIDTH],
            store_sem.at[half],
        )
        copy.start()
        stores[half] = copy

    def lanes(half):
        return slice(half * WIDTH, half * WIDTH + WIDTH)

    own = (first_sum, sums)
    from_plane = (first_plane, plane_slots)
    along_line = (first_line, line_slots)

    def to_plane(group):
        settle(along_line[0] if group else outgoing, other_send.at[0])
        for index, step in enumerate(plane):
            push(
                own[group].at[0],
                from_plane[group].at[index],
                other_send.at[0],
                other_recv.at[1 + group],
                step,
            )

    def to_line(group):
        with jax.named_scope("w_plane%d" % group):
            settle(from_plane[group], other_recv.at[1 + group])
        own[group][1] = own[group][0] + jnp.sum(from_plane[group][...], axis=0)
        settle(from_plane[group], other_send.at[0])
        for index, step in enumerate(line):
            push(
                own[group].at[1],
                along_line[group].at[index],
                other_send.at[0],
                other_recv.at[3 + group],
                step,
            )

    def from_line(group):
        with jax.named_scope("w_line%d" % group):
            settle(along_line[group], other_recv.at[3 + group])
        return own[group][1] + jnp.sum(along_line[group][...], axis=0)

    for half in range(HALVES):
        keep_copy(ext.at[0, half, 1:5, 1:5, 1:5], zeroth_ref, 0, half)
    with jax.named_scope("inner"):
        build(groups[:2], 0, lambda k, offset: shifted[k])
        matrix_hi[...], matrix_lo[...] = turned(pick, slice(0, 256))
        side_matrix(0, 0)
        for half in range(HALVES):
            before(0, half)
    for half in range(HALVES):
        first_sum[0, :, :, lanes(half)] = product(core(0, half), core(0, half))[None]
    to_plane(0)
    with jax.named_scope("w_coef"):
        settle(incoming, other_recv.at[0])
    with jax.named_scope("rim"):
        build(groups[2:], 352, mirrored)
        for axis, side in ((0, 1), (1, 0), (1, 1), (2, 0), (2, 1)):
            side_matrix(axis, side)

    for half in range(HALVES):
        advance(0, half, inner(1, half))
        exchange(1, half)
        keep_copy(ext.at[1, half, 1:5, 1:5, 1:5], first_ref, 1, half)
        before(1, half)
        if half == 0:
            to_line(0)
        sums[0, 0, :, lanes(half)] = product(core(0, half), core(1, half))
        sums[0, 1, :, lanes(half)] = product(core(1, half), core(1, half))
    for half in range(HALVES):
        advance(1, half, inner(2, half))
        exchange(2, half)
        keep_copy(ext.at[2, half, 1:5, 1:5, 1:5], second_ref, 2, half)
        before(2, half)
        sums[0, 2, :, lanes(half)] = product(core(0, half), core(2, half))
        sums[0, 3, :, lanes(half)] = product(core(1, half), core(2, half))
        sums[0, 4, :, lanes(half)] = product(core(2, half), core(2, half))
    to_plane(1)
    g00 = from_line(0)[0]
    for half in range(HALVES):
        advance(2, half, last.at[half])
        final_sum[half] = product(core(2, half), last[half])
        settle(halo_like(2), halo_send.at[half])
        for index, step in enumerate(others):
            if half == HALVES - 1 and index == 60:
                to_line(1)
            push(
                final_sum.at[half],
                final_slots.at[half, index],
                halo_send.at[half],
                final_recv.at[half],
                step,
            )
        keep_copy(last.at[half], third_ref, 3, half)
    rest = from_line(1)
    rr2, pq, weight, start, along = early_part(
        g00, rest[0], rest[2], rest[1], rest[3], rest[4], shift[...] + CENTRE
    )
    with jax.named_scope("w_stores"):
        for copy in stores:
            copy.wait()
        settle(along_line[1], other_send.at[0])
    totals = []
    for half in range(HALVES):
        with jax.named_scope("w_final%d" % half):
            settle(final_slots.at[half], final_recv.at[half])
        totals.append(final_sum[half] + jnp.sum(final_slots[half], axis=0))
    a2 = rr2 / (pq + weight * jnp.concatenate(totals, axis=1))
    for n in range(7):
        mix_ref[n : n + 1, :] = start[n] + a2 * along[n]
    for half in range(HALVES):
        settle(final_slots.at[half], halo_send.at[half])


def combine(zeroth_ref, first_ref, second_ref, third_ref, mix_ref, sol_ref, res_ref, sol, res, sem):
    for part in [(slice(x, x + 1), slice(y, y + 2)) for x in range(4) for y in (0, 2)]:
        zeroth, first, second = zeroth_ref[part], first_ref[part], second_ref[part]
        res[part] = (
            mix_ref[3] * zeroth
            + mix_ref[4] * first
            + mix_ref[5] * second
            + mix_ref[6] * third_ref[part]
        )
        pltpu.make_async_copy(res.at[part], res_ref.at[part], sem.at[1]).start()
        sol[part] = mix_ref[0] * zeroth + mix_ref[1] * first + mix_ref[2] * second
        pltpu.make_async_copy(sol.at[part], sol_ref.at[part], sem.at[0]).start()
    pltpu.make_async_copy(sol, sol_ref, sem.at[0]).wait()
    pltpu.make_async_copy(res, res_ref, sem.at[1]).wait()


def solution(mesh):
    sizes = tuple(mesh.shape[name] for name in AXES)
    count = sizes[0] * sizes[1] * sizes[2]

    def per_device(right_side, bond_blocks, bond_open, onsite_blocks, orbital_levels, column_shift):
        vmem = pl.BlockSpec(memory_space=pltpu.VMEM)
        hbm = pl.BlockSpec(memory_space=pl.ANY)
        out = jax.ShapeDtypeStruct((4, 4, 4, 4, 256), f32)
        field = pltpu.VMEM((4, 4, 4, 4, 256), f32)
        kept = pl.pallas_call(
            functools.partial(kernel, sizes),
            out_shape=(field,) * 4 + (pltpu.VMEM((7, 256), f32),),
            in_specs=[hbm] * 6,
            out_specs=(hbm,) * 4 + (vmem,),
            scratch_shapes=[
                pltpu.VMEM((3, HALVES, 6, 6, 6, 4, WIDTH), f32),
                pltpu.VMEM((HALVES, 4, 4, 4, 4, WIDTH), f32),
                pltpu.VMEM((HALVES, 4, 4, 4, 4, WIDTH), f32),
                pltpu.VMEM((4, 4, 4, 4, WIDTH), f32),
                pltpu.VMEM((4, 4, 4, 4, 4, 13), f32),
                pltpu.VMEM((4, 4, 4, 13), jnp.int32),
                pltpu.VMEM((4, 4, 4, 4, 4), f32),
                pltpu.VMEM((4, 4, 4, 4), f32),
                pltpu.VMEM((1, 256), f32),
                pltpu.VMEM((16, 4, 256), f32),
                pltpu.VMEM((16, 4, 256), f32),
                pltpu.VMEM((16, 4, 256), f32),
                pltpu.VMEM((CARGO, 4, 256), f32),
                pltpu.VMEM((CARGO, 4, 256), f32),
                pltpu.VMEM((864, 256), f32),
                pltpu.VMEM((256, 256), bf16),
                pltpu.VMEM((256, 256), bf16),
                pltpu.VMEM((2, 64, 288), bf16),
                pltpu.VMEM((2, 64, 192), bf16),
                pltpu.VMEM((2, 64, 432), bf16),
                pltpu.VMEM((2, 1, 1, 256), f32),
                pltpu.VMEM((sizes[0] * sizes[1] - 1, 1, 1, 256), f32),
                pltpu.VMEM((sizes[2] - 1, 1, 1, 256), f32),
                pltpu.VMEM((2, 5, 1, 256), f32),
                pltpu.VMEM((sizes[0] * sizes[1] - 1, 5, 1, 256), f32),
                pltpu.VMEM((sizes[2] - 1, 5, 1, 256), f32),
                pltpu.VMEM((HALVES, 1, WIDTH), f32),
                pltpu.VMEM((HALVES, count - 1, 1, WIDTH), f32),
                pltpu.SemaphoreType.DMA((5,)),
                pltpu.SemaphoreType.DMA((HALVES,)),
                pltpu.SemaphoreType.DMA((HALVES,)),
                pltpu.SemaphoreType.DMA((2, HALVES, 2)),
                pltpu.SemaphoreType.DMA((1,)),
                pltpu.SemaphoreType.DMA((5,)),
                pltpu.SemaphoreType.DMA((HALVES,)),
            ],
            compiler_params=pltpu.CompilerParams(collective_id=0, has_side_effects=True),
        )(
            right_side,
            jnp.transpose(bond_blocks, (1, 2, 3, 4, 5, 0)),
            jnp.transpose(bond_open, (1, 2, 3, 0)),
            onsite_blocks,
            orbital_levels,
            column_shift.reshape(1, 256),
        )
        return pl.pallas_call(
            combine,
            out_shape=(out, out),
            in_specs=[vmem] * 5,
            out_specs=(hbm, hbm),
            scratch_shapes=[
                pltpu.VMEM((4, 4, 4, 4, 256), f32),
                pltpu.VMEM((4, 4, 4, 4, 256), f32),
                pltpu.SemaphoreType.DMA((2,)),
            ],
        )(*[pltpu.with_memory_space_constraint(value, pltpu.VMEM) for value in kept])

    return jax.shard_map(
        per_device,
        mesh=mesh,
        in_specs=(
            P("gx", "gy", "gz", None, None),
            P(None, None, None, "gx", "gy", "gz"),
            P(None, "gx", "gy", "gz"),
            P(None, None, "gx", "gy", "gz"),
            P(None, "gx", "gy", "gz"),
            P(),
        ),
        out_specs=(P("gx", "gy", "gz", None, None), P("gx", "gy", "gz", None, None)),
        check_vma=False,
    )
```

```python
import functools

import jax
import jax.numpy as jnp
from jax import lax
from jax.experimental import pallas as pl
from jax.experimental.pallas import tpu as pltpu
from jax.sharding import PartitionSpec as P

f32 = jnp.float32
bf16 = jnp.bfloat16
MESH = pl.DeviceIdType.MESH

CENTRE = 1.95
GAMMA1 = 0.65 * 0.65 / 3.0
GAMMA2 = 0.65 * 0.65 * 4.0 / 15.0
HALVES = 2
WIDTH = 256 // HALVES
AXES = ("gx", "gy", "gz")

ALL = (-1, 0, 1)
every = [(i, j, k) for i in ALL for j in ALL for k in ALL]
half_offsets = [o for o in every if o > (0, 0, 0)]
directions = sorted(
    [o for o in every if o != (0, 0, 0)],
    key=lambda d: (-abs(d[2]), abs(d[0]) + abs(d[1])),
)
hops = sorted(
    {
        tuple(o[n] * keep[n] for n in range(3))
        for o in half_offsets
        for keep in [(i, j, k) for i in (0, 1) for j in (0, 1) for k in (0, 1)]
    }
    - {(0, 0, 0)},
    key=lambda d: (-abs(d[2]), d),
)
cargo = {
    hop: [
        k
        for k, o in enumerate(half_offsets)
        if all(hop[n] in (0, o[n]) for n in range(3))
    ]
    for hop in hops
}
cargo_slot, slabs = {}, []
cargo_start = {}
for hop in hops:
    cargo_start[hop] = len(slabs)
    for index, k in enumerate(cargo[hop]):
        if index % 4 == 0:
            slabs.append((hop, []))
        slabs[-1][1].append(k)
        cargo_slot[hop, k] = (len(slabs) - 1, index % 4)
CARGO = len(slabs)

INSIDE = range(0, 4)
WITH_RIM = range(-1, 5)
groups = [
    (INSIDE, INSIDE, INSIDE),
    ((4,), WITH_RIM, INSIDE),
    ((-1,), WITH_RIM, INSIDE),
    (INSIDE, (-1,), INSIDE),
    (INSIDE, (4,), INSIDE),
    (WITH_RIM, WITH_RIM, (-1,)),
    (WITH_RIM, WITH_RIM, (4,)),
]


def span_of(step, side):
    if step == 0:
        return slice(1, 5)
    if side == "source":
        return slice(4, 5) if step > 0 else slice(1, 2)
    return slice(0, 1) if step > 0 else slice(5, 6)


def reach(values):
    return slice(values[0] + 1, values[-1] + 2)


def split(value):
    high = value.astype(bf16)
    return high, (value - high.astype(f32)).astype(bf16)


def early_part(g00, g01, g02, g11, g12, g22, theta):
    g03 = g12 - GAMMA2 * g01
    g13 = g22 + GAMMA1 * g02 - GAMMA2 * g11
    a0 = g00 / (theta * g00 + g01)
    s0 = a0
    r0, r1 = 1.0 - a0 * theta, -a0
    rr1 = r0 * r0 * g00 + 2.0 * r0 * r1 * g01 + r1 * r1 * g11
    p0, p1 = r0 + rr1 / g00, r1
    q0, q1, q2 = theta * p0 + GAMMA1 * p1, p0 + theta * p1, p1
    pq = p0 * (q0 * g00 + q1 * g01 + q2 * g02) + p1 * (q0 * g01 + q1 * g11 + q2 * g12)
    a1 = rr1 / pq
    s0, s1 = s0 + a1 * p0, a1 * p1
    r0, r1, r2 = r0 - a1 * q0, r1 - a1 * q1, -a1 * q2
    rr2 = (
        r0 * (r0 * g00 + r1 * g01 + r2 * g02)
        + r1 * (r0 * g01 + r1 * g11 + r2 * g12)
        + r2 * (r0 * g02 + r1 * g12 + r2 * g22)
    )
    ratio = rr2 / rr1
    p0, p1, p2 = r0 + ratio * p0, r1 + ratio * p1, r2
    q0 = theta * p0 + GAMMA1 * p1
    q1 = p0 + theta * p1 + GAMMA2 * p2
    q2 = p1 + theta * p2
    q3 = p2
    pq = (
        p0 * (q0 * g00 + q1 * g01 + q2 * g02 + q3 * g03)
        + p1 * (q0 * g01 + q1 * g11 + q2 * g12 + q3 * g13)
        + p2 * (q0 * g02 + q1 * g12 + q2 * g22)
    )
    return rr2, pq, p2 * q3, (s0, s1, 0.0, r0, r1, r2, 0.0), (p0, p1, p2, -q0, -q1, -q2, -q3)


def kernel(
    sizes,
    right_ref,
    bond_ref,
    open_ref,
    onsite_ref,
    level_ref,
    shift_ref,
    zeroth_ref,
    first_ref,
    second_ref,
    third_ref,
    mix_ref,
    ext,
    last,
    partial,
    diag,
    bonds,
    opened,
    onsite,
    levels,
    shift,
    natural,
    flipped,
    shifted,
    outgoing,
    incoming,
    matrix_t,
    matrix_hi,
    matrix_lo,
    matrix_x,
    matrix_y,
    matrix_z,
    first_sum,
    first_plane,
    first_line,
    sums,
    plane_slots,
    line_slots,
    final_sum,
    final_slots,
    load_sem,
    store_sem,
    halo_send,
    halo_recv,
    other_send,
    other_recv,
    final_recv,
):
    me = [lax.axis_index(name) for name in AXES]
    side_refs = (matrix_x, matrix_y, matrix_z)

    def at(step):
        return tuple(lax.rem(me[n] + (step[n] + sizes[n]), sizes[n]) for n in range(3))

    def push(source, target, send, recv, step):
        pltpu.make_async_remote_copy(
            src_ref=source,
            dst_ref=target,
            send_sem=send,
            recv_sem=recv,
            device_id=at(step),
            device_id_type=MESH,
        ).start()

    def settle(like, sem):
        pltpu.make_async_copy(like, like, sem).wait()

    plane = [(i, j, 0) for i in range(sizes[0]) for j in range(sizes[1]) if (i, j) != (0, 0)]
    line = [(0, 0, k) for k in range(1, sizes[2])]
    others = [
        (i, j, k)
        for i in range(sizes[0])
        for j in range(sizes[1])
        for k in range(sizes[2])
        if (i, j, k) != (0, 0, 0)
    ]
    far = {0: 0, 1: 3, 2: 4, 3: 3, 4: 2}

    def path(step):
        return -(min(step[1], sizes[1] - step[1]) + far.get(min(step[2], sizes[2] - step[2]), 4))

    others.sort(key=path)
    greeted = {tuple(d[n] % sizes[n] for n in range(3)) for d in directions}
    greeted = sorted(greeted | set(plane) | set(line), key=lambda d: (path(d), d))


    loads = []
    for half in range(HALVES):
        loads.append(
            pltpu.make_async_copy(
                right_ref.at[:, :, :, :, half * WIDTH : half * WIDTH + WIDTH],
                ext.at[0, half, 1:5, 1:5, 1:5],
                store_sem.at[half],
            )
        )
    tables = [
        pltpu.make_async_copy(bond_ref, bonds, load_sem.at[0]),
        pltpu.make_async_copy(open_ref, opened, load_sem.at[1]),
        pltpu.make_async_copy(onsite_ref, onsite, load_sem.at[2]),
        pltpu.make_async_copy(level_ref, levels, load_sem.at[3]),
        pltpu.make_async_copy(shift_ref, shift, load_sem.at[4]),
    ]
    for copy in tables + loads:
        copy.start()
    barrier = pltpu.get_barrier_semaphore()
    with jax.named_scope("greet"):
        for step in greeted:
            pl.semaphore_signal(barrier, inc=1, device_id=at(step), device_id_type=MESH)

    lane = lax.broadcasted_iota(jnp.int32, (4, 256), 1)
    place = ((lane >> 4) & 3, (lane >> 2) & 3, lane & 3)

    def cyclic(value, axis, step):
        stride = (16, 4, 1)[axis]
        if step == 0:
            return value
        if step > 0:
            return jnp.where(
                place[axis] == 0,
                pltpu.roll(value, 256 - 3 * stride, 1),
                pltpu.roll(value, stride, 1),
            )
        return jnp.where(
            place[axis] == 3,
            pltpu.roll(value, 3 * stride, 1),
            pltpu.roll(value, 256 - stride, 1),
        )

    def layer(hop):
        axis = [n for n in range(3) if hop[n]][0]
        return axis, (16, 4, 1)[axis], 0 if hop[axis] > 0 else 3

    def packed(hop, values):
        axis, stride, edge = layer(hop)
        total = values[0]
        for index in range(1, len(values)):
            spot = (edge + index) % 4
            moved = pltpu.roll(values[index], (stride * (spot - edge)) % 256, 1)
            total = jnp.where(place[axis] == spot, moved, total)
        return total

    def unpacked(hop, k):
        axis, stride, edge = layer(hop)
        slot, index = cargo_slot[hop, k]
        spot = (edge + index) % 4
        value = incoming[slot]
        return value if index == 0 else pltpu.roll(value, (stride * (edge - spot)) % 256, 1)

    with jax.named_scope("tables"):
        for copy in tables:
            copy.wait()
        blocks = bonds[...] * opened[...].astype(f32)
        table = blocks.reshape(1024, 13).T
        for orb in range(4):
            natural[0:13, orb, :] = table[:, 256 * orb : 256 * orb + 256]
        table = jnp.swapaxes(blocks, 0, 1).reshape(1024, 13).T
        for orb in range(4):
            flipped[0:13, orb, :] = table[:, 256 * orb : 256 * orb + 256]
        for k, offset in enumerate(half_offsets):
            value = natural[k]
            for axis in range(3):
                value = cyclic(value, axis, offset[axis])
            shifted[k] = value
        for slot, (hop, blocks) in enumerate(slabs):
            outgoing[slot] = packed(hop, [shifted[k] for k in blocks])

    def exchange(number, half, parts=(1, 0)):
        if number:
            settle(halo_like(2), halo_send.at[half])
        for step in directions:
            part = 1 if step[2] else 0
            if part not in parts:
                continue
            push(
                ext.at[(number, half) + tuple(span_of(s, "source") for s in step)],
                ext.at[(number, half) + tuple(span_of(s, "target") for s in step)],
                halo_send.at[half],
                halo_recv.at[number % 2, half, part],
                step,
            )

    def halo_like(part):
        return matrix_t.at[0 : (80, 72, 152)[part] * 4 * WIDTH // 256]

    with jax.named_scope("w_barrier"):
        pl.semaphore_wait(barrier, len(greeted))
    for hop in hops:
        count = sum(1 for slab in slabs if slab[0] == hop)
        rows = slice(cargo_start[hop], cargo_start[hop] + count)
        push(outgoing.at[rows], incoming.at[rows], other_send.at[0], other_recv.at[0], hop)
    loads[0].wait()
    exchange(0, 0)

    out_row = lax.broadcasted_iota(jnp.int32, (256, 256), 0)
    out_lane = lax.broadcasted_iota(jnp.int32, (256, 256), 1)
    same = ((out_row & 3) == (out_lane >> 6)) & ((out_row >> 2) == (out_lane & 63))
    pick = jnp.where(same, 1.0, 0.0).astype(bf16)

    with jax.named_scope("onsite"):
        spread = jnp.where(
            lax.broadcasted_iota(jnp.int32, (4, 256), 0) == (lane & 3), 1.0, 0.0
        )
        raw = onsite[...]
        raw = (0.5 * (raw + jnp.swapaxes(raw, 0, 1))).reshape(256, 4)
        wide = jnp.dot(
            raw, spread, precision=lax.Precision.HIGHEST, preferred_element_type=f32
        )
        keep = ((out_row >> 6) == (out_lane >> 6)) & (
            (out_row & 15) == ((out_lane >> 2) & 15)
        )
        wide = jnp.where(keep, wide, 0.0).reshape(4, 4, 16, 256)
        local = jnp.sum(jnp.sum(wide, axis=0), axis=1)
        wide = jnp.dot(
            levels[...].reshape(64, 4) - CENTRE,
            spread,
            precision=lax.Precision.HIGHEST,
            preferred_element_type=f32,
        )
        keep = out_row[0:64] == (out_lane[0:64] >> 2)
        level = jnp.sum(jnp.where(keep, wide, 0.0), axis=0, keepdims=True)
        level = jnp.sum(jnp.where(same, level, 0.0), axis=1, keepdims=True)
        diag[...] = jnp.broadcast_to(level, (256, WIDTH)).reshape(4, 4, 4, 4, WIDTH)

    for half in range(1, HALVES):
        loads[half].wait()
        exchange(0, half)

    near = [
        [(place[axis] >= e - 1) & (place[axis] <= e + 1) for e in WITH_RIM]
        for axis in range(3)
    ]

    def turned(chooser, span):
        across = (((1,), (1,)), ((), ()))
        return [
            lax.dot_general(chooser, part, across, preferred_element_type=f32).astype(bf16)
            for part in split(matrix_t[span, :])
        ]

    def build(chosen, first_row, behind):
        table = {(0, 0, 0): local}
        for k, offset in enumerate(half_offsets):
            table[offset] = flipped[k]
            table[tuple(-o for o in offset)] = behind(k, offset)
        for axis in range(3):
            kind = jnp.where(place[axis] == 3, 0, place[axis])
            fresh = {}
            for key in table:
                picks = []
                for residue in range(3):
                    step = (key[axis] % 3 - residue + 1) % 3 - 1
                    picks.append(table[key[:axis] + (step,) + key[axis + 1 :]])
                fresh[key] = jnp.where(
                    kind == 0, picks[0], jnp.where(kind == 1, picks[1], picks[2])
                )
            table = fresh
        row = first_row
        for group in chosen:
            for ex in group[0]:
                for ey in group[1]:
                    both = near[0][ex + 1] & near[1][ey + 1]
                    for ez in group[2]:
                        key = tuple((e + 1) % 3 - 1 for e in (ex, ey, ez))
                        matrix_t[row : row + 4, :] = jnp.where(
                            both & near[2][ez + 1], table[key], 0.0
                        )
                        row += 4

    layers = (((3, 5), (0, 0)), ((0, 0), (3, 5)), ((0, 0), (3, 5)))
    starts = ((256, 352, 448), (448, 512, 576), (576, 720, 864))

    def side_matrix(axis, side):
        row, at_lane = out_row[0:64], out_lane[0:64]
        x, y, z = (at_lane >> 4) & 3, (at_lane >> 2) & 3, at_lane & 3
        along = ((y, z), (x, z), (x, y))[axis]
        chooser = (
            ((row & 3) == (at_lane >> 6))
            & ((row >> 4) == along[0])
            & (((row >> 2) & 3) == along[1])
            & ((x, y, z)[axis] == layers[axis][side][0])
        )
        first, end = starts[axis][side : side + 2]
        high, low = turned(jnp.where(chooser, 1.0, 0.0).astype(bf16), slice(first, end))
        for index, part in enumerate((high, low, high)):
            span = slice((end - first) * index, (end - first) * (index + 1))
            side_refs[axis][side, :, span] = part

    def mirrored(k, offset):
        axes = [n for n in range(3) if offset[n]]

        def choose(position, hop):
            if position == len(axes):
                return unpacked(hop, k) if any(hop) else shifted[k]
            axis = axes[position]
            edge = 0 if offset[axis] > 0 else 3
            away = hop[:axis] + (offset[axis],) + hop[axis + 1 :]
            return jnp.where(
                place[axis] == edge, choose(position + 1, away), choose(position + 1, hop)
            )

        return choose(0, (0, 0, 0))

    def times(span, value):
        high, low = split(value)
        return (
            jnp.dot(matrix_hi[:, span], low, preferred_element_type=f32)
            + jnp.dot(matrix_lo[:, span], high, preferred_element_type=f32)
            + jnp.dot(matrix_hi[:, span], high, preferred_element_type=f32)
        )

    def core(number, half):
        return ext[number, half, 1:5, 1:5, 1:5]

    def before(number, half):
        total = times(slice(0, 256), core(number, half).reshape(256, WIDTH))
        total = total.reshape(4, 4, 4, 4, WIDTH) + diag[...] * core(number, half)
        if number:
            total = total - (GAMMA1, GAMMA2)[number - 1] * core(number - 1, half)
        partial[half] = total

    def arrive(number, half, part):
        with jax.named_scope("w_halo%d_%d" % (2 * number + half, part)):
            settle(halo_like(part), halo_recv.at[number % 2, half, part])

    def advance(number, half, target):
        def add(axis):
            for side in range(2):
                out, rim = layers[axis][side]
                where = [slice(None)] * 3
                where[axis] = out
                if axis == 0:
                    value = ext[number, half, rim, :, 1:5]
                elif axis == 1:
                    value = ext[number, half, 1:5, rim, 1:5]
                else:
                    value = ext[number, half, :, :, rim]
                high, low = split(value.reshape(-1, WIDTH))
                part = jnp.dot(
                    side_refs[axis][side],
                    jnp.concatenate([low, high, high], axis=0),
                    preferred_element_type=f32,
                )
                target[tuple(where)] += part.reshape(4, 4, 4, WIDTH)

        target[...] = partial[half]
        arrive(number, half, 0)
        add(0)
        add(1)
        arrive(number, half, 1)
        add(2)

    def inner(number, half):
        return ext.at[number, half, 1:5, 1:5, 1:5]

    def product(left, right):
        return jnp.sum(jnp.sum(left * right, axis=(0, 1, 2)), axis=0, keepdims=True)

    stores = [None] * HALVES

    def keep_copy(source, target, number, half):
        if number:
            stores[half].wait()
        copy = pltpu.make_async_copy(
            source,
            target.at[:, :, :, :, half * WIDTH : half * WIDTH + WIDTH],
            store_sem.at[half],
        )
        copy.start()
        stores[half] = copy

    def lanes(half):
        return slice(half * WIDTH, half * WIDTH + WIDTH)

    own = (first_sum, sums)
    from_plane = (first_plane, plane_slots)
    along_line = (first_line, line_slots)

    def to_plane(group):
        settle(along_line[0] if group else outgoing, other_send.at[0])
        for index, step in enumerate(plane):
            push(
                own[group].at[0],
                from_plane[group].at[index],
                other_send.at[0],
                other_recv.at[1 + group],
                step,
            )

    def to_line(group):
        with jax.named_scope("w_plane%d" % group):
            settle(from_plane[group], other_recv.at[1 + group])
        own[group][1] = own[group][0] + jnp.sum(from_plane[group][...], axis=0)
        settle(from_plane[group], other_send.at[0])
        for index, step in enumerate(line):
            push(
                own[group].at[1],
                along_line[group].at[index],
                other_send.at[0],
                other_recv.at[3 + group],
                step,
            )

    def from_line(group):
        with jax.named_scope("w_line%d" % group):
            settle(along_line[group], other_recv.at[3 + group])
        return own[group][1] + jnp.sum(along_line[group][...], axis=0)

    for half in range(HALVES):
        keep_copy(ext.at[0, half, 1:5, 1:5, 1:5], zeroth_ref, 0, half)
    with jax.named_scope("inner"):
        build(groups[:2], 0, lambda k, offset: shifted[k])
        matrix_hi[...], matrix_lo[...] = turned(pick, slice(0, 256))
        side_matrix(0, 0)
        for half in range(HALVES):
            before(0, half)
    for half in range(HALVES):
        first_sum[0, :, :, lanes(half)] = product(core(0, half), core(0, half))[None]
    to_plane(0)
    with jax.named_scope("w_coef"):
        settle(incoming, other_recv.at[0])
    with jax.named_scope("rim"):
        build(groups[2:], 352, mirrored)
        for axis, side in ((0, 1), (1, 0), (1, 1), (2, 0), (2, 1)):
            side_matrix(axis, side)

    for half in range(HALVES):
        advance(0, half, inner(1, half))
        exchange(1, half)
        keep_copy(ext.at[1, half, 1:5, 1:5, 1:5], first_ref, 1, half)
        before(1, half)
        if half == 0:
            to_line(0)
        sums[0, 0, :, lanes(half)] = product(core(0, half), core(1, half))
        sums[0, 1, :, lanes(half)] = product(core(1, half), core(1, half))
    for half in range(HALVES):
        advance(1, half, inner(2, half))
        exchange(2, half)
        keep_copy(ext.at[2, half, 1:5, 1:5, 1:5], second_ref, 2, half)
        before(2, half)
        sums[0, 2, :, lanes(half)] = product(core(0, half), core(2, half))
        sums[0, 3, :, lanes(half)] = product(core(1, half), core(2, half))
        sums[0, 4, :, lanes(half)] = product(core(2, half), core(2, half))
    to_plane(1)
    g00 = from_line(0)[0]
    for half in range(HALVES):
        advance(2, half, last.at[half])
        final_sum[half] = product(core(2, half), last[half])
        settle(halo_like(2), halo_send.at[half])
        for index, step in enumerate(others):
            if half == HALVES - 1 and index == 60:
                to_line(1)
            push(
                final_sum.at[half],
                final_slots.at[half, index],
                halo_send.at[half],
                final_recv.at[half],
                step,
            )
        keep_copy(last.at[half], third_ref, 3, half)
    rest = from_line(1)
    rr2, pq, weight, start, along = early_part(
        g00, rest[0], rest[2], rest[1], rest[3], rest[4], shift[...] + CENTRE
    )
    with jax.named_scope("w_stores"):
        for copy in stores:
            copy.wait()
        settle(along_line[1], other_send.at[0])
    totals = []
    for half in range(HALVES):
        with jax.named_scope("w_final%d" % half):
            settle(final_slots.at[half], final_recv.at[half])
        totals.append(final_sum[half] + jnp.sum(final_slots[half], axis=0))
    a2 = rr2 / (pq + weight * jnp.concatenate(totals, axis=1))
    for n in range(7):
        mix_ref[n : n + 1, :] = start[n] + a2 * along[n]
    for half in range(HALVES):
        settle(final_slots.at[half], halo_send.at[half])


def combine(zeroth_ref, first_ref, second_ref, third_ref, mix_ref, sol_ref, res_ref, sol, res, sem):
    for part in [(slice(x, x + 1), slice(y, y + 2)) for x in range(4) for y in (0, 2)]:
        zeroth, first, second = zeroth_ref[part], first_ref[part], second_ref[part]
        res[part] = (
            mix_ref[3] * zeroth
            + mix_ref[4] * first
            + mix_ref[5] * second
            + mix_ref[6] * third_ref[part]
        )
        pltpu.make_async_copy(res.at[part], res_ref.at[part], sem.at[1]).start()
        sol[part] = mix_ref[0] * zeroth + mix_ref[1] * first + mix_ref[2] * second
        pltpu.make_async_copy(sol.at[part], sol_ref.at[part], sem.at[0]).start()
    pltpu.make_async_copy(sol, sol_ref, sem.at[0]).wait()
    pltpu.make_async_copy(res, res_ref, sem.at[1]).wait()


def solution(mesh):
    sizes = tuple(mesh.shape[name] for name in AXES)
    count = sizes[0] * sizes[1] * sizes[2]

    def per_device(right_side, bond_blocks, bond_open, onsite_blocks, orbital_levels, column_shift):
        vmem = pl.BlockSpec(memory_space=pltpu.VMEM)
        hbm = pl.BlockSpec(memory_space=pl.ANY)
        out = jax.ShapeDtypeStruct((4, 4, 4, 4, 256), f32)
        field = pltpu.VMEM((4, 4, 4, 4, 256), f32)
        kept = pl.pallas_call(
            functools.partial(kernel, sizes),
            out_shape=(field,) * 4 + (pltpu.VMEM((7, 256), f32),),
            in_specs=[hbm] * 6,
            out_specs=(hbm,) * 4 + (vmem,),
            scratch_shapes=[
                pltpu.VMEM((3, HALVES, 6, 6, 6, 4, WIDTH), f32),
                pltpu.VMEM((HALVES, 4, 4, 4, 4, WIDTH), f32),
                pltpu.VMEM((HALVES, 4, 4, 4, 4, WIDTH), f32),
                pltpu.VMEM((4, 4, 4, 4, WIDTH), f32),
                pltpu.VMEM((4, 4, 4, 4, 4, 13), f32),
                pltpu.VMEM((4, 4, 4, 13), jnp.int32),
                pltpu.VMEM((4, 4, 4, 4, 4), f32),
                pltpu.VMEM((4, 4, 4, 4), f32),
                pltpu.VMEM((1, 256), f32),
                pltpu.VMEM((16, 4, 256), f32),
                pltpu.VMEM((16, 4, 256), f32),
                pltpu.VMEM((16, 4, 256), f32),
                pltpu.VMEM((CARGO, 4, 256), f32),
                pltpu.VMEM((CARGO, 4, 256), f32),
                pltpu.VMEM((864, 256), f32),
                pltpu.VMEM((256, 256), bf16),
                pltpu.VMEM((256, 256), bf16),
                pltpu.VMEM((2, 64, 288), bf16),
                pltpu.VMEM((2, 64, 192), bf16),
                pltpu.VMEM((2, 64, 432), bf16),
                pltpu.VMEM((2, 1, 1, 256), f32),
                pltpu.VMEM((sizes[0] * sizes[1] - 1, 1, 1, 256), f32),
                pltpu.VMEM((sizes[2] - 1, 1, 1, 256), f32),
                pltpu.VMEM((2, 5, 1, 256), f32),
                pltpu.VMEM((sizes[0] * sizes[1] - 1, 5, 1, 256), f32),
                pltpu.VMEM((sizes[2] - 1, 5, 1, 256), f32),
                pltpu.VMEM((HALVES, 1, WIDTH), f32),
                pltpu.VMEM((HALVES, count - 1, 1, WIDTH), f32),
                pltpu.SemaphoreType.DMA((5,)),
                pltpu.SemaphoreType.DMA((HALVES,)),
                pltpu.SemaphoreType.DMA((HALVES,)),
                pltpu.SemaphoreType.DMA((2, HALVES, 2)),
                pltpu.SemaphoreType.DMA((1,)),
                pltpu.SemaphoreType.DMA((5,)),
                pltpu.SemaphoreType.DMA((HALVES,)),
            ],
            compiler_params=pltpu.CompilerParams(collective_id=0, has_side_effects=True),
        )(
            right_side,
            jnp.transpose(bond_blocks, (1, 2, 3, 4, 5, 0)),
            jnp.transpose(bond_open, (1, 2, 3, 0)),
            onsite_blocks,
            orbital_levels,
            column_shift.reshape(1, 256),
        )
        return pl.pallas_call(
            combine,
            out_shape=(out, out),
            in_specs=[vmem] * 5,
            out_specs=(hbm, hbm),
            scratch_shapes=[
                pltpu.VMEM((4, 4, 4, 4, 256), f32),
                pltpu.VMEM((4, 4, 4, 4, 256), f32),
                pltpu.SemaphoreType.DMA((2,)),
            ],
        )(*[pltpu.with_memory_space_constraint(value, pltpu.VMEM) for value in kept])

    return jax.shard_map(
        per_device,
        mesh=mesh,
        in_specs=(
            P("gx", "gy", "gz", None, None),
            P(None, None, None, "gx", "gy", "gz"),
            P(None, "gx", "gy", "gz"),
            P(None, None, "gx", "gy", "gz"),
            P(None, "gx", "gy", "gz"),
            P(),
        ),
        out_specs=(P("gx", "gy", "gz", None, None), P("gx", "gy", "gz", None, None)),
        check_vma=False,
    )
```
